32 devices in a mesh: sample: 2 (over y), gz: 4 (over x, core), gy: 4 (over z).
Axes of the slice: x: 2, y: 2, z: 4, core: 2. Of those that a mesh axis runs over, the one named last changes fastest.
Arguments:
- right_side: float32 [64, 64, 256], P(('sample', 'gz'), 'gy'), parts along dimension 0, may hold values from -8 to 8
- labels: int32 [8, 8, 32], P(('sample', 'gz'), 'gy'), parts along dimension 0, may hold values from 0 to 7
- region_coeff: float32 [16], P('sample'), parts along dimension 0, may hold values from 0.2 to 5
- shift_index: int32 [16], P('sample'), parts along dimension 0, may hold values from 0 to 15
- shift_table: float32 [16], replicated, may hold values from 0.1 to 4
- time_step: float32 [2], P('sample'), parts along dimension 0, may hold values from 0.3 to 1
- block_inverse: float32 [8, 128, 128], replicated, as said below
Outputs:
- solution: float32 [8, 64, 64, 256], P(None, ('sample', 'gz'), 'gy'), parts along dimension 1
- residual: float32 [8, 64, 64, 256], P(None, ('sample', 'gz'), 'gy'), parts along dimension 1
The draws below stay inside these ranges and needn't reach their ends.
There are 2 independent parts, one for each index of `sample`. The reference program is written for one: setup_inputs(seed, part) draws one part's arguments, and reference() takes and returns one part's arrays. A program takes and returns all parts, laid end to end along the dimension named above; an argument that names none is the same for every part. Nothing has to cross between parts.
Inputs may be any that keep to these rules, and one draw needn't show every extreme that they name: `shift_index`: a table row for each system. `labels`: a region for each block. `block_inverse`: each block is symmetric and positive definite.
All inputs are finite; a program needn't handle non-finite values.
Results may differ from the reference program's by a relative error of at most 0.00022.
Values sent between devices are 32-bit elements; how exact they have to be, the bound alone decides.
A program may use at most 64 MiB of HBM per device.

```python
import math
import jax
import jax.numpy as jnp
from jax import lax

NX = 256
SHIFTS = 8
ITERS = 2
BLOCK = 128
REGIONS = 8
SHIFT_TABLE = 16
NZ = 32
NY = 64


def draw_block_inverse(key, part):
    first_key = jax.random.fold_in(key, 11)
    second_key = jax.random.fold_in(key, 23)
    diagonal_part = jax.random.uniform(first_key, (SHIFTS, BLOCK), jnp.float32, 1.0, 1.6)
    noise = jax.random.normal(second_key, (SHIFTS, BLOCK, BLOCK), jnp.float32) * (0.3 / math.sqrt(BLOCK))
    symmetric = (noise + jnp.swapaxes(noise, 1, 2)) / math.sqrt(2.0)
    return symmetric + diagonal_part[:, :, None] * jnp.eye(BLOCK, dtype=jnp.float32)[None]


def place_ends(array, key, low, top_value):
    index_at = [jax.random.randint(jax.random.fold_in(key, axis), (), 0, length) for axis, length in enumerate(array.shape)]
    widest = array.shape.index(max(array.shape))
    beside = index_at[:widest] + [(index_at[widest] + 1) % array.shape[widest]] + index_at[widest + 1:]
    return array.at[tuple(index_at)].set(low).at[tuple(beside)].set(top_value)


def level_of(own_key, dims, shards, low, largest):
    loudness, own = 1.0, jax.random.fold_in(own_key, 6)
    for dim, shards_of in shards:
        heights = jnp.exp(jax.random.uniform(jax.random.fold_in(own, dim), (shards_of,), jnp.float32, low / len(shards), largest / len(shards)))
        loudness = loudness * jnp.repeat(heights, dims[dim] // shards_of).reshape([-1 if axis == dim else 1 for axis in range(len(dims))])
    return loudness


def scatter_about(own_key, dims, scale, most, cuts=(), held_as=jnp.bfloat16):
    drawn = scale * jax.random.normal(own_key, dims, jnp.float32)
    if cuts:
        drawn = drawn * level_of(own_key, dims, cuts, -0.22, 0.18)
    return jnp.clip(drawn, -most, most).astype(held_as)


def setup_inputs(seed: int = 0, part: int = 0) -> dict:
    key_list = jax.random.split(jax.random.key(seed), 8)
    part_keys = jax.random.split(jax.random.fold_in(key_list[7], part), 8)
    return {
        "right_side": scatter_about(part_keys[0], (NZ, NY, NX), 1.0, 8.0, ((0, 4), (1, 4)), jnp.float32),
        "labels": place_ends(jax.random.randint(part_keys[1], (NZ // 8, NY // 8, NX // 8), 0, REGIONS), jax.random.fold_in(part_keys[1], 1), 0, REGIONS - 1).astype(jnp.int32),
        "region_coeff": jnp.clip(jnp.exp(jax.random.uniform(part_keys[2], (REGIONS,), jnp.float32, math.log(0.2), math.log(5.0))), 0.2, 5.0),
        "shift_index": place_ends(jax.random.randint(part_keys[3], (SHIFTS,), 0, SHIFT_TABLE), jax.random.fold_in(part_keys[3], 1), 0, SHIFT_TABLE - 1).astype(jnp.int32),
        "shift_table": jnp.clip(jnp.exp(jax.random.uniform(key_list[4], (SHIFT_TABLE,), jnp.float32, math.log(0.1), math.log(4.0))), 0.1, 4.0),
        "time_step": jnp.clip(jnp.exp(jax.random.uniform(part_keys[5], (1,), jnp.float32, math.log(0.3), math.log(1.0))), 0.3, 1.0),
        "block_inverse": draw_block_inverse(jax.random.fold_in(key_list[7], 71), part),
    }


NEIGHBOURS = [(step_z, step_y, step_x, 0.5 ** (abs(step_z) + abs(step_y) + abs(step_x) - 1))
              for step_z in (-1, 0, 1) for step_y in (-1, 0, 1) for step_x in (-1, 0, 1)
              if (step_z, step_y, step_x) != (0, 0, 0)]


def cell_values(labels, region_coeff):
    picked = jnp.where(labels[..., None] == jnp.arange(region_coeff.shape[0]).astype(jnp.int32), region_coeff, 0.0)
    table = jnp.sum(picked, axis=-1)
    return jnp.repeat(jnp.repeat(jnp.repeat(table, 8, 0), 8, 1), 8, 2)


def stencil(field, padded, conductivity, padded_cond):
    depth, rows, width = field.shape[-3], field.shape[-2], field.shape[-1]
    total = jnp.zeros_like(field)
    for step_z, step_y, step_x, weight in NEIGHBOURS:
        beside = padded[..., 1 + step_z:1 + step_z + depth, 1 + step_y:1 + step_y + rows, 1 + step_x:1 + step_x + width]
        cond_beside = padded_cond[1 + step_z:1 + step_z + depth, 1 + step_y:1 + step_y + rows, 1 + step_x:1 + step_x + width]
        total = total + (weight * 0.5) * (conductivity + cond_beside) * (field - beside)
    return total


def precondition(residual, inverse):
    shape = residual.shape
    blocks = residual.reshape(shape[0], shape[1], shape[2] // BLOCK, BLOCK)
    result = jnp.einsum("zyxb,bc->zyxc", blocks, inverse, precision=lax.Precision.HIGHEST)
    return result.reshape(shape)


def reference(right_side, labels, region_coeff, shift_index, shift_table, time_step, block_inverse):
    conductivity = cell_values(labels, region_coeff)
    padded_cond = jnp.pad(conductivity, 1)
    shift_values = jnp.sum(jnp.where(shift_index[:, None] == jnp.arange(SHIFT_TABLE).astype(jnp.int32), shift_table, 0.0), axis=1)

    def solve(operands):
        shift_value, inverse = operands

        def apply_system(field):
            return shift_value * field + time_step[0] * stencil(field, jnp.pad(field, 1), conductivity, padded_cond)

        solution = jnp.zeros_like(right_side)
        residual = right_side
        precond = precondition(residual, inverse)
        direction = precond
        rz_now = jnp.sum(residual * precond)
        for iteration in range(ITERS):
            image = apply_system(direction)
            alpha = rz_now / jnp.sum(direction * image)
            solution = solution + alpha * direction
            residual = residual - alpha * image
            precond = precondition(residual, inverse)
            rz_next = jnp.sum(residual * precond)
            direction = precond + (rz_next / rz_now) * direction
            rz_now = rz_next
        return solution, residual

    solutions, residuals = lax.map(solve, (shift_values, block_inverse))
    return solutions, residuals
```

```python
import functools

import jax
import jax.numpy as jnp
from jax import lax
from jax.experimental import pallas as pl
from jax.experimental.pallas import tpu as pltpu
from jax.sharding import PartitionSpec as P

MESH = pl.DeviceIdType.MESH
EDGE = 8
REACH = 2
DIRECTIONS = [(dz, dy) for dz in (-1, 0, 1) for dy in (-1, 0, 1) if (dz, dy) != (0, 0)]


def slot(dz, dy):
    return (dz + 1) * 3 + dy + 1


def split(x):
    high = x.astype(jnp.bfloat16)
    low = (x - high.astype(jnp.float32)).astype(jnp.bfloat16)
    return high, low


def smooth_x(parts):
    width = parts[0].shape[1]
    lane = lax.broadcasted_iota(jnp.int32, parts[0].shape, 1)
    first, last = lane == 0, lane == width - 1
    rolled = [pltpu.roll(u, 1, 1) for u in parts]
    pairs = [
        u + jnp.where(first, rolled[i - 1] if i else 0.0, rolled[i]) for i, u in enumerate(parts)
    ]
    rolled = [pltpu.roll(h, width - 1, 1) for h in pairs]
    return [
        h + jnp.where(last, rolled[i + 1] if i + 1 < len(pairs) else parts[i], rolled[i])
        for i, h in enumerate(pairs)
    ]


def smooth_y(u):
    h = u + pltpu.roll(u, 1, 0)
    return h + pltpu.roll(h, u.shape[0] - 1, 0)


def smooth_xy(parts):
    return [smooth_y(u) for u in smooth_x(parts)]


def kernel(
    grid,
    right_ref,
    labels_ref,
    coeff_ref,
    index_ref,
    table_ref,
    step_ref,
    inverse_ref,
    solution_ref,
    residual_ref,
    r_ext,
    p_ext,
    q_ext,
    w_ext,
    y_own,
    weights,
    c_rows,
    label_rows,
    c_planes,
    diag,
    y_send,
    z_recv,
    y_recv,
    corner_recv,
    label_recv,
    message,
    gathered,
    coefs,
    out_s,
    out_r,
    send_sem,
    recv_sem,
    label_send_sem,
    label_recv_sem,
    gather_send_sem,
    gather_recv_sem,
    out_sem,
):
    n_gz, n_gy = grid
    group = n_gz * n_gy
    depth, rows, nx = right_ref.shape
    systems, lanes = inverse_ref.shape[0], inverse_ref.shape[1]
    halves = nx // lanes
    ring = r_ext.shape[2]
    y_blocks = labels_ref.shape[1]
    label_cols = labels_ref.shape[2]
    sample, gz, gy = lax.axis_index("sample"), lax.axis_index("gz"), lax.axis_index("gy")
    me = gz * n_gy + gy

    def has(dz, dy):
        z_ok = gz + dz >= 0 if dz < 0 else gz + dz < n_gz
        y_ok = gy + dy >= 0 if dy < 0 else gy + dy < n_gy
        return jnp.logical_and(z_ok, y_ok)

    def present(dz, dy):
        return jnp.where(has(dz, dy), 1.0, 0.0).astype(jnp.float32)

    def peer_of(offset):
        peer = lax.rem(me + offset, group)
        return peer, (sample, lax.div(peer, n_gy), lax.rem(peer, n_gy))

    z_recv[...] = jnp.zeros_like(z_recv)
    y_recv[...] = jnp.zeros_like(y_recv)
    corner_recv[...] = jnp.zeros_like(corner_recv)
    label_recv[...] = jnp.zeros_like(label_recv)
    y_send[0] = right_ref[:, 0:REACH, :]
    y_send[1] = right_ref[:, rows - REACH : rows, :]

    barrier = pltpu.get_barrier_semaphore()

    def greet(offset, carry):
        _, device = peer_of(offset)
        pl.semaphore_signal(barrier, inc=1, device_id=device, device_id_type=MESH)
        return carry

    lax.fori_loop(1, group, greet, 0)

    for m in range(systems):
        high, low = split(inverse_ref[m])
        weights[m, 0:lanes, 0:lanes] = high
        weights[m, lanes : 2 * lanes, 0:lanes] = high
        weights[m, 0:lanes, lanes : 2 * lanes] = low
        weights[m, lanes : 2 * lanes, lanes : 2 * lanes] = low
    r_ext[...] = jnp.zeros_like(r_ext)
    for h in range(halves):
        r_ext[h, REACH : REACH + depth, 0:rows, :] = right_ref[:, :, h * lanes : (h + 1) * lanes]

    pl.semaphore_wait(barrier, group - 1)

    def halo_copy(dz, dy):
        device = (sample, gz + dz, gy + dy)
        z_from = depth - REACH if dz > 0 else 0
        if dy == 0:
            source = right_ref.at[pl.ds(z_from, REACH)]
            target = z_recv.at[0 if dz > 0 else 1]
        elif dz == 0:
            source = y_send.at[1 if dy > 0 else 0]
            target = y_recv.at[0 if dy > 0 else 1]
        else:
            source = y_send.at[1 if dy > 0 else 0, pl.ds(z_from, REACH)]
            target = corner_recv.at[0 if dz > 0 else 1, 0 if dy > 0 else 1]
        return pltpu.make_async_remote_copy(
            src_ref=source,
            dst_ref=target,
            send_sem=send_sem.at[slot(dz, dy)],
            recv_sem=recv_sem.at[slot(-dz, -dy)],
            device_id=device,
            device_id_type=MESH,
        )

    def label_copy(dz, dy):
        return pltpu.make_async_remote_copy(
            src_ref=labels_ref,
            dst_ref=label_recv.at[slot(-dz, -dy)],
            send_sem=label_send_sem.at[slot(dz, dy)],
            recv_sem=label_recv_sem.at[slot(-dz, -dy)],
            device_id=(sample, gz + dz, gy + dy),
            device_id_type=MESH,
        )

    for dz, dy in DIRECTIONS:

        @pl.when(has(dz, dy))
        def _(dz=dz, dy=dy):
            label_copy(dz, dy).start()
            halo_copy(dz, dy).start()

    for dz, dy in DIRECTIONS:

        @pl.when(has(dz, dy))
        def _(dz=dz, dy=dy):
            label_copy(-dz, -dy).wait_recv()
            halo_copy(-dz, -dy).wait_recv()

    for h in range(halves):
        cut = slice(h * lanes, (h + 1) * lanes)
        for side in (0, 1):
            planes = slice(0, REACH) if side == 0 else slice(REACH + depth, 2 * REACH + depth)
            r_ext[h, planes, 0:rows, :] = z_recv[side, :, :, cut]
            r_ext[h, planes, rows : rows + REACH, :] = corner_recv[side, 1, :, :, cut]
            r_ext[h, planes, ring - REACH : ring, :] = corner_recv[side, 0, :, :, cut]
        own = slice(REACH, REACH + depth)
        r_ext[h, own, rows : rows + REACH, :] = y_recv[1, :, :, cut]
        r_ext[h, own, ring - REACH : ring, :] = y_recv[0, :, :, cut]

    label_rows[...] = jnp.zeros_like(label_rows)
    for s in range(9):
        table = labels_ref[0] if s == slot(0, 0) else label_recv[s, 0]
        label_rows[s * y_blocks : (s + 1) * y_blocks, :] = table.astype(jnp.float32)
    spread = jnp.where(
        lax.broadcasted_iota(jnp.int32, (label_cols, nx), 0)
        == lax.broadcasted_iota(jnp.int32, (label_cols, nx), 1) // EDGE,
        1.0,
        0.0,
    ).astype(jnp.bfloat16)
    wide = jnp.dot(
        label_rows[...].astype(jnp.bfloat16), spread, preferred_element_type=jnp.float32
    )
    cells = jnp.zeros_like(wide)
    scale = step_ref[0] * 0.125
    for region in range(coeff_ref.shape[0]):
        cells = jnp.where(wide == float(region), coeff_ref[region] * scale, cells)
    c_rows[...] = cells

    sub = lax.broadcasted_iota(jnp.int32, (EDGE, lanes), 0)
    for dz in (-1, 0, 1):
        for h in range(halves):
            cut = slice(h * lanes, (h + 1) * lanes)

            def row(dy, block):
                at = slot(dz, dy) * y_blocks + block
                value = c_rows[at : at + 1, cut]
                if (dz, dy) != (0, 0):
                    value = value * present(dz, dy)
                return jnp.broadcast_to(value, (EDGE, lanes))

            for block in range(y_blocks):
                c_planes[dz + 1, h, block * EDGE : (block + 1) * EDGE, :] = row(0, block)
            c_planes[dz + 1, h, rows:ring, :] = jnp.where(
                sub < EDGE // 2, row(1, 0), row(-1, y_blocks - 1)
            )

    smooth = [smooth_xy([c_planes[d, h] for h in range(halves)]) for d in range(3)]
    for h in range(halves):
        low, own, high = (smooth[d][h] for d in range(3))
        diag[0, h] = 3.0 * low + own + 64.0 * c_planes[0, h]
        diag[1, h] = low + 3.0 * own + 64.0 * c_planes[1, h]
        diag[2, h] = 4.0 * own + 64.0 * c_planes[1, h]
        diag[3, h] = high + 3.0 * own + 64.0 * c_planes[1, h]
        diag[4, h] = 3.0 * high + own + 64.0 * c_planes[2, h]

    ring_row = lax.broadcasted_iota(jnp.int32, (ring, lanes), 0)
    row_mask = jnp.where(
        ring_row < rows,
        1.0,
        jnp.where(ring_row < rows + EDGE // 2, present(0, 1), present(0, -1)),
    )

    def apply(field, z, shift):
        def c_of(plane):
            return 0 if plane < 0 else 2 if plane >= depth else 1

        below, here, above = field(z - 1), field(z), field(z + 1)
        kind = 0 if z < 0 else 4 if z >= depth else 1 if z == 0 else 3 if z == depth - 1 else 2
        ku, kcu = [], []
        for h in range(halves):
            u = (below[h] + here[h]) + (here[h] + above[h])
            if kind == 2:
                cu = c_planes[1, h] * u
            else:
                cu = (
                    c_planes[c_of(z - 1), h] * below[h]
                    + 2.0 * (c_planes[c_of(z), h] * here[h])
                    + c_planes[c_of(z + 1), h] * above[h]
                )
            ku.append(u)
            kcu.append(cu)
        ku, kcu = smooth_xy(ku), smooth_xy(kcu)
        return [
            (diag[kind, h] + shift) * here[h] - c_planes[c_of(z), h] * ku[h] - kcu[h]
            for h in range(halves)
        ]

    def product(x, m):
        shape = x.shape
        flat = x.reshape(-1, lanes)
        high, low = split(flat)
        both = jnp.dot(
            jnp.concatenate([high, low], axis=1), weights[m], preferred_element_type=jnp.float32
        )
        return (both[:, 0:lanes] + both[:, lanes : 2 * lanes]).reshape(shape)

    def fold(total, term):
        term = term.reshape(-1, 8, lanes)
        for i in range(term.shape[0]):
            total = total + term[i]
        return total

    def put(quantity, m, total):
        value = jnp.sum(jnp.sum(total, axis=0, keepdims=True), axis=1, keepdims=True)
        coefs[quantity, pl.ds(m, 1), :] = jnp.broadcast_to(value, (1, lanes))

    zero = jnp.zeros((8, lanes), jnp.float32)

    def first(m, carry):
        shift = table_ref[index_ref[m]]
        p_ext[m] = product(r_ext[...], m)
        a, c = zero, zero
        for z in range(-1, depth + 1):
            image = apply(
                lambda k: [p_ext[m, h, k + REACH] for h in range(halves)], z, shift
            )
            for h in range(halves):
                value = image[h] * row_mask
                if z < 0:
                    value = value * present(-1, 0)
                elif z >= depth:
                    value = value * present(1, 0)
                else:
                    p = p_ext[m, h, z + REACH, 0:rows, :]
                    a = fold(a, p * r_ext[h, z + REACH, 0:rows, :])
                    c = fold(c, p * value[0:rows])
                q_ext[m, h, z + 1] = value
        put(0, m, a)
        put(1, m, c)
        return carry

    lax.fori_loop(0, systems, first, 0)

    a_own, c_own = coefs[0], coefs[1]
    sigma = jnp.where(a_own > 0.0, c_own / jnp.where(a_own > 0.0, a_own, 1.0), 0.0)
    coefs[5] = sigma

    def second(m, carry):
        shift = table_ref[index_ref[m]]
        s_row = coefs[5, pl.ds(m, 1), :]
        q_shifted = q_ext[m] - s_row[None, None] * r_ext[:, 1 : REACH + depth + 1]
        w_ext[m] = product(q_shifted, m)
        g, f, e = zero, zero, zero
        for z in range(depth):
            image = apply(lambda k: [w_ext[m, h, k + 1] for h in range(halves)], z, shift)
            for h in range(halves):
                y = image[h][0:rows]
                w = w_ext[m, h, z + 1, 0:rows, :]
                q = q_ext[m, h, z + 1, 0:rows, :] - s_row * r_ext[h, z + REACH, 0:rows, :]
                g = fold(g, w * q)
                f = fold(f, p_ext[m, h, z + REACH, 0:rows, :] * y)
                e = fold(e, w * y)
                y_own[m, h, z] = y
        put(2, m, g)
        put(3, m, f)
        put(4, m, e)
        return carry

    lax.fori_loop(0, systems, second, 0)

    lane = lax.broadcasted_iota(jnp.int32, (systems, lanes), 1)
    packed = coefs[0]
    for quantity in range(1, 6):
        packed = jnp.where(lane == quantity, coefs[quantity], packed)
    message[...] = packed
    gathered[me] = packed

    def gather_copy(device, source):
        return pltpu.make_async_remote_copy(
            src_ref=message,
            dst_ref=gathered.at[source],
            send_sem=gather_send_sem.at[source],
            recv_sem=gather_recv_sem.at[source],
            device_id=device,
            device_id_type=MESH,
        )

    def send_to(offset):
        peer, device = peer_of(offset)
        return pltpu.make_async_remote_copy(
            src_ref=message,
            dst_ref=gathered.at[me],
            send_sem=gather_send_sem.at[peer],
            recv_sem=gather_recv_sem.at[me],
            device_id=device,
            device_id_type=MESH,
        )

    def send_step(offset, carry):
        send_to(offset).start()
        return carry

    lax.fori_loop(1, group, send_step, 0)

    def receive_step(offset, carry):
        peer, device = peer_of(offset)
        gather_copy(device, peer).wait_recv()
        return carry

    lax.fori_loop(1, group, receive_step, 0)

    def column(source, quantity):
        return jnp.broadcast_to(
            gathered[source][:, quantity : quantity + 1], (systems, lanes)
        )

    a_all = [column(d, 0) for d in range(group)]
    c_all = [column(d, 1) for d in range(group)]
    rz_0, curvature_0 = sum(a_all), sum(c_all)
    alpha_0 = rz_0 / curvature_0
    kept = [1.0 - alpha_0 * column(d, 5) for d in range(group)]
    g_all = [column(d, 2) for d in range(group)]
    rz_1 = sum(
        kept[d] * kept[d] * a_all[d] + alpha_0 * alpha_0 * g_all[d] for d in range(group)
    )
    beta = rz_1 / rz_0
    curvature_1 = zero
    for d in range(group):
        k = kept[d] + beta
        curvature_1 = curvature_1 + (
            k * k * c_all[d]
            - alpha_0 * k * (column(d, 3) + g_all[d])
            + alpha_0 * alpha_0 * column(d, 4)
        )
    alpha_1 = rz_1 / curvature_1
    own_k = 1.0 - alpha_0 * sigma + beta
    coefs[0] = alpha_0 + alpha_1 * own_k
    coefs[1] = alpha_0 * alpha_1

    def out_copies(m):
        return (
            pltpu.make_async_copy(out_s.at[m], solution_ref.at[m], out_sem.at[0, m]),
            pltpu.make_async_copy(out_r.at[m], residual_ref.at[m], out_sem.at[1, m]),
        )

    def finish(m, carry):
        main = coefs[0, pl.ds(m, 1), :][None]
        side = coefs[1, pl.ds(m, 1), :][None]
        own = slice(REACH, REACH + depth)
        for h in range(halves):
            cut = slice(h * lanes, (h + 1) * lanes)
            out_s[m, :, :, cut] = (
                main * p_ext[m, h, own, 0:rows, :] - side * w_ext[m, h, 1 : depth + 1, 0:rows, :]
            )
            out_r[m, :, :, cut] = (
                right_ref[:, :, cut]
                - main * q_ext[m, h, 1 : depth + 1, 0:rows, :]
                + side * y_own[m, h]
            )
        for copy in out_copies(m):
            copy.start()
        return carry

    lax.fori_loop(0, systems, finish, 0)

    def close_out(m, carry):
        for copy in out_copies(m):
            copy.wait()
        return carry

    lax.fori_loop(0, systems, close_out, 0)

    def close_send(offset, carry):
        send_to(offset).wait_send()
        return carry

    lax.fori_loop(1, group, close_send, 0)
    for dz, dy in DIRECTIONS:

        @pl.when(has(dz, dy))
        def _(dz=dz, dy=dy):
            label_copy(dz, dy).wait_send()
            halo_copy(dz, dy).wait_send()


def on_device(
    grid, right_side, labels, region_coeff, shift_index, shift_table, time_step, block_inverse
):
    depth, rows, nx = right_side.shape
    systems, lanes = block_inverse.shape[0], block_inverse.shape[1]
    halves = nx // lanes
    assert depth == EDGE and labels.shape[0] == 1
    group = grid[0] * grid[1]
    ring = rows + EDGE
    y_blocks = labels.shape[1]
    label_pad = -(-9 * y_blocks // 8) * 8
    f32 = jnp.float32
    vmem = pl.BlockSpec(memory_space=pltpu.VMEM)
    smem = pl.BlockSpec(memory_space=pltpu.SMEM)
    hbm = pl.BlockSpec(memory_space=pl.ANY)
    out = jax.ShapeDtypeStruct((systems,) + right_side.shape, f32)
    dma = pltpu.SemaphoreType.DMA
    return pl.pallas_call(
        functools.partial(kernel, grid),
        out_shape=(out, out),
        in_specs=[vmem, vmem, smem, smem, smem, smem, vmem],
        out_specs=(hbm, hbm),
        scratch_shapes=[
            pltpu.VMEM((halves, depth + 2 * REACH, ring, lanes), f32),
            pltpu.VMEM((systems, halves, depth + 2 * REACH, ring, lanes), f32),
            pltpu.VMEM((systems, halves, depth + 2, ring, lanes), f32),
            pltpu.VMEM((systems, halves, depth + 2, ring, lanes), f32),
            pltpu.VMEM((systems, halves, depth, rows, lanes), f32),
            pltpu.VMEM((systems, 2 * lanes, 2 * lanes), jnp.bfloat16),
            pltpu.VMEM((label_pad, nx), f32),
            pltpu.VMEM((label_pad, labels.shape[2]), f32),
            pltpu.VMEM((3, halves, ring, lanes), f32),
            pltpu.VMEM((5, halves, ring, lanes), f32),
            pltpu.VMEM((2, depth, REACH, nx), f32),
            pltpu.VMEM((2, REACH, rows, nx), f32),
            pltpu.VMEM((2, depth, REACH, nx), f32),
            pltpu.VMEM((2, 2, REACH, REACH, nx), f32),
            pltpu.VMEM((9,) + labels.shape, jnp.int32),
            pltpu.VMEM((systems, lanes), f32),
            pltpu.VMEM((group, systems, lanes), f32),
            pltpu.VMEM((6, systems, lanes), f32),
            pltpu.VMEM(out.shape, f32),
            pltpu.VMEM(out.shape, f32),
            dma((9,)),
            dma((9,)),
            dma((9,)),
            dma((9,)),
            dma((group,)),
            dma((group,)),
            dma((2, systems)),
        ],
        compiler_params=pltpu.CompilerParams(
            collective_id=0, has_side_effects=True, vmem_limit_bytes=40 * 1024 * 1024
        ),
    )(right_side, labels, region_coeff, shift_index, shift_table, time_step, block_inverse)


def solution(mesh):
    in_specs = (
        P(("sample", "gz"), "gy", None),
        P(("sample", "gz"), "gy", None),
        P("sample"),
        P("sample"),
        P(),
        P("sample"),
        P(),
    )
    out_specs = (P(None, ("sample", "gz"), "gy", None), P(None, ("sample", "gz"), "gy", None))
    grid = (mesh.shape["gz"], mesh.shape["gy"])
    return jax.shard_map(
        functools.partial(on_device, grid),
        mesh=mesh,
        in_specs=in_specs,
        out_specs=out_specs,
        check_vma=False,
    )
```

```python
import functools

import jax
import jax.numpy as jnp
from jax import lax
from jax.experimental import pallas as pl
from jax.experimental.pallas import tpu as pltpu
from jax.sharding import PartitionSpec as P

MESH = pl.DeviceIdType.MESH
EDGE = 8
REACH = 2
DIRECTIONS = [(dz, dy) for dz in (-1, 0, 1) for dy in (-1, 0, 1) if (dz, dy) != (0, 0)]


def slot(dz, dy):
    return (dz + 1) * 3 + dy + 1


def split(x):
    high = x.astype(jnp.bfloat16)
    low = (x - high.astype(jnp.float32)).astype(jnp.bfloat16)
    return high, low


def smooth_x(parts):
    width = parts[0].shape[1]
    lane = lax.broadcasted_iota(jnp.int32, parts[0].shape, 1)
    first, last = lane == 0, lane == width - 1
    rolled = [pltpu.roll(u, 1, 1) for u in parts]
    pairs = [
        u + jnp.where(first, rolled[i - 1] if i else 0.0, rolled[i]) for i, u in enumerate(parts)
    ]
    rolled = [pltpu.roll(h, width - 1, 1) for h in pairs]
    return [
        h + jnp.where(last, rolled[i + 1] if i + 1 < len(pairs) else parts[i], rolled[i])
        for i, h in enumerate(pairs)
    ]


def smooth_y(u):
    h = u + pltpu.roll(u, 1, 0)
    return h + pltpu.roll(h, u.shape[0] - 1, 0)


def smooth_xy(parts):
    return [smooth_y(u) for u in smooth_x(parts)]


def kernel(
    grid,
    right_hbm,
    labels_hbm,
    coeff_hbm,
    index_hbm,
    table_hbm,
    step_hbm,
    inverse_hbm,
    r_ext,
    p_ext,
    q_ext,
    w_ext,
    y_own,
    coefs,
    right_ref,
    labels_ref,
    coeff_ref,
    index_ref,
    table_ref,
    step_ref,
    inverse_ref,
    weights,
    c_rows,
    label_rows,
    c_planes,
    diag,
    y_send,
    z_recv,
    y_recv,
    corner_recv,
    label_recv,
    message,
    gathered,
    load_sem,
    near_sem,
    send_sem,
    recv_sem,
    label_send_sem,
    label_recv_sem,
    gather_send_sem,
    gather_recv_sem,
):
    n_gz, n_gy = grid
    group = n_gz * n_gy
    depth, rows, nx = right_ref.shape
    systems, lanes = inverse_ref.shape[0], inverse_ref.shape[1]
    halves = nx // lanes
    ring = r_ext.shape[2]
    y_blocks = labels_ref.shape[1]
    label_cols = labels_ref.shape[2]
    sample, gz, gy = lax.axis_index("sample"), lax.axis_index("gz"), lax.axis_index("gy")
    me = gz * n_gy + gy

    def has(dz, dy):
        z_ok = gz + dz >= 0 if dz < 0 else gz + dz < n_gz
        y_ok = gy + dy >= 0 if dy < 0 else gy + dy < n_gy
        return jnp.logical_and(z_ok, y_ok)

    def present(dz, dy):
        return jnp.where(has(dz, dy), 1.0, 0.0).astype(jnp.float32)

    def peer_of(offset):
        peer = lax.rem(me + offset, group)
        return peer, (sample, lax.div(peer, n_gy), lax.rem(peer, n_gy))

    loads = [
        pltpu.make_async_copy(source, target, load_sem.at[i])
        for i, (source, target) in enumerate(
            (
                (right_hbm, right_ref),
                (labels_hbm, labels_ref),
                (inverse_hbm, inverse_ref),
                (coeff_hbm, coeff_ref),
                (step_hbm, step_ref),
                (index_hbm, index_ref),
                (table_hbm, table_ref),
            )
        )
    ]
    for load in loads:
        load.start()

    z_recv[...] = jnp.zeros_like(z_recv)
    y_recv[...] = jnp.zeros_like(y_recv)
    corner_recv[...] = jnp.zeros_like(corner_recv)
    label_recv[...] = jnp.zeros_like(label_recv)

    barrier = pltpu.get_barrier_semaphore()

    def signal_near(semaphore):
        for dz, dy in DIRECTIONS:

            @pl.when(has(dz, dy))
            def _(dz=dz, dy=dy):
                pl.semaphore_signal(
                    semaphore,
                    inc=1,
                    device_id=(sample, gz + dz, gy + dy),
                    device_id_type=MESH,
                )

    z_near = 1 + (gz > 0).astype(jnp.int32) + (gz < n_gz - 1).astype(jnp.int32)
    y_near = 1 + (gy > 0).astype(jnp.int32) + (gy < n_gy - 1).astype(jnp.int32)
    near = z_near * y_near - 1

    signal_near(barrier)
    r_ext[...] = jnp.zeros_like(r_ext)
    loads[0].wait()
    loads[1].wait()
    y_send[0] = right_ref[:, 0:REACH, :]
    y_send[1] = right_ref[:, rows - REACH : rows, :]
    for h in range(halves):
        r_ext[h, REACH : REACH + depth, 0:rows, :] = right_ref[:, :, h * lanes : (h + 1) * lanes]

    pl.semaphore_wait(barrier, near)

    def halo_copy(dz, dy):
        device = (sample, gz + dz, gy + dy)
        z_from = depth - REACH if dz > 0 else 0
        if dy == 0:
            source = right_ref.at[pl.ds(z_from, REACH)]
            target = z_recv.at[0 if dz > 0 else 1]
        elif dz == 0:
            source = y_send.at[1 if dy > 0 else 0]
            target = y_recv.at[0 if dy > 0 else 1]
        else:
            source = y_send.at[1 if dy > 0 else 0, pl.ds(z_from, REACH)]
            target = corner_recv.at[0 if dz > 0 else 1, 0 if dy > 0 else 1]
        return pltpu.make_async_remote_copy(
            src_ref=source,
            dst_ref=target,
            send_sem=send_sem.at[slot(dz, dy)],
            recv_sem=recv_sem.at[slot(-dz, -dy)],
            device_id=device,
            device_id_type=MESH,
        )

    def label_copy(dz, dy):
        return pltpu.make_async_remote_copy(
            src_ref=labels_ref,
            dst_ref=label_recv.at[slot(-dz, -dy)],
            send_sem=label_send_sem.at[slot(dz, dy)],
            recv_sem=label_recv_sem.at[slot(-dz, -dy)],
            device_id=(sample, gz + dz, gy + dy),
            device_id_type=MESH,
        )

    for dz, dy in DIRECTIONS:

        @pl.when(has(dz, dy))
        def _(dz=dz, dy=dy):
            label_copy(dz, dy).start()
            halo_copy(dz, dy).start()

    for load in loads[2:]:
        load.wait()
    for m in range(systems):
        high, low = split(inverse_ref[m])
        weights[m, 0:lanes, 0:lanes] = high
        weights[m, lanes : 2 * lanes, 0:lanes] = high
        weights[m, 0:lanes, lanes : 2 * lanes] = low
        weights[m, lanes : 2 * lanes, lanes : 2 * lanes] = low

    def pieces(x):
        return jnp.concatenate(split(x.reshape(-1, lanes)), axis=1)

    def product(x, m):
        both = jnp.dot(x, weights[m], preferred_element_type=jnp.float32)
        return both[:, 0:lanes] + both[:, lanes : 2 * lanes]

    own_planes = slice(REACH, REACH + depth)
    own_pieces = pieces(r_ext[:, own_planes, 0:rows, :])
    for m in range(systems):
        p_ext[m, :, own_planes, 0:rows, :] = product(own_pieces, m).reshape(
            halves, depth, rows, lanes
        )

    for dz, dy in DIRECTIONS:

        @pl.when(has(dz, dy))
        def _(dz=dz, dy=dy):
            label_copy(-dz, -dy).wait_recv()
            halo_copy(-dz, -dy).wait_recv()

    rounds = max(n_gz, n_gy) - 3
    if rounds > 0:
        signal_near(near_sem.at[0])

    for h in range(halves):
        cut = slice(h * lanes, (h + 1) * lanes)
        for side in (0, 1):
            planes = slice(0, REACH) if side == 0 else slice(REACH + depth, 2 * REACH + depth)
            r_ext[h, planes, 0:rows, :] = z_recv[side, :, :, cut]
            r_ext[h, planes, rows : rows + REACH, :] = corner_recv[side, 1, :, :, cut]
            r_ext[h, planes, ring - REACH : ring, :] = corner_recv[side, 0, :, :, cut]
        own = slice(REACH, REACH + depth)
        r_ext[h, own, rows : rows + REACH, :] = y_recv[1, :, :, cut]
        r_ext[h, own, ring - REACH : ring, :] = y_recv[0, :, :, cut]

    label_rows[...] = jnp.zeros_like(label_rows)
    for s in range(9):
        table = labels_ref[0] if s == slot(0, 0) else label_recv[s, 0]
        label_rows[s * y_blocks : (s + 1) * y_blocks, :] = table.astype(jnp.float32)
    spread = jnp.where(
        lax.broadcasted_iota(jnp.int32, (label_cols, nx), 0)
        == lax.broadcasted_iota(jnp.int32, (label_cols, nx), 1) // EDGE,
        1.0,
        0.0,
    ).astype(jnp.bfloat16)
    wide = jnp.dot(
        label_rows[...].astype(jnp.bfloat16), spread, preferred_element_type=jnp.float32
    )
    cells = jnp.zeros_like(wide)
    scale = step_ref[0] * 0.125
    for region in range(coeff_ref.shape[0]):
        cells = jnp.where(wide == float(region), coeff_ref[region] * scale, cells)
    c_rows[...] = cells

    sub = lax.broadcasted_iota(jnp.int32, (EDGE, lanes), 0)
    for dz in (-1, 0, 1):
        for h in range(halves):
            cut = slice(h * lanes, (h + 1) * lanes)

            def row(dy, block):
                at = slot(dz, dy) * y_blocks + block
                value = c_rows[at : at + 1, cut]
                if (dz, dy) != (0, 0):
                    value = value * present(dz, dy)
                return jnp.broadcast_to(value, (EDGE, lanes))

            for block in range(y_blocks):
                c_planes[dz + 1, h, block * EDGE : (block + 1) * EDGE, :] = row(0, block)
            c_planes[dz + 1, h, rows:ring, :] = jnp.where(
                sub < EDGE // 2, row(1, 0), row(-1, y_blocks - 1)
            )

    smooth = [smooth_xy([c_planes[d, h] for h in range(halves)]) for d in range(3)]
    for h in range(halves):
        low, own, high = (smooth[d][h] for d in range(3))
        diag[0, h] = 3.0 * low + own + 64.0 * c_planes[0, h]
        diag[1, h] = low + 3.0 * own + 64.0 * c_planes[1, h]
        diag[2, h] = 4.0 * own + 64.0 * c_planes[1, h]
        diag[3, h] = high + 3.0 * own + 64.0 * c_planes[1, h]
        diag[4, h] = 3.0 * high + own + 64.0 * c_planes[2, h]

    ring_row = lax.broadcasted_iota(jnp.int32, (ring, lanes), 0)
    row_mask = jnp.where(
        ring_row < rows,
        1.0,
        jnp.where(ring_row < rows + EDGE // 2, present(0, 1), present(0, -1)),
    )

    def apply(field, z, shift):
        def c_of(plane):
            return 0 if plane < 0 else 2 if plane >= depth else 1

        below, here, above = field(z - 1), field(z), field(z + 1)
        kind = 0 if z < 0 else 4 if z >= depth else 1 if z == 0 else 3 if z == depth - 1 else 2
        ku, kcu = [], []
        for h in range(halves):
            u = (below[h] + here[h]) + (here[h] + above[h])
            if kind == 2:
                cu = c_planes[1, h] * u
            else:
                cu = (
                    c_planes[c_of(z - 1), h] * below[h]
                    + 2.0 * (c_planes[c_of(z), h] * here[h])
                    + c_planes[c_of(z + 1), h] * above[h]
                )
            ku.append(u)
            kcu.append(cu)
        ku, kcu = smooth_xy(ku), smooth_xy(kcu)
        return [
            (diag[kind, h] + shift) * here[h] - c_planes[c_of(z), h] * ku[h] - kcu[h]
            for h in range(halves)
        ]

    def fold(total, term):
        term = term.reshape(-1, 8, lanes)
        for i in range(term.shape[0]):
            total = total + term[i]
        return total

    def put(quantity, m, total):
        value = jnp.sum(jnp.sum(total, axis=0, keepdims=True), axis=1, keepdims=True)
        coefs[quantity, pl.ds(m, 1), :] = jnp.broadcast_to(value, (1, lanes))

    zero = jnp.zeros((8, lanes), jnp.float32)

    z_pieces = [
        pieces(r_ext[:, planes])
        for planes in (slice(0, REACH), slice(REACH + depth, 2 * REACH + depth))
    ]
    y_pieces = pieces(r_ext[:, own_planes, rows:ring, :])
    for m in range(systems):
        for planes, x in zip(
            (slice(0, REACH), slice(REACH + depth, 2 * REACH + depth)), z_pieces
        ):
            p_ext[m, :, planes] = product(x, m).reshape(halves, REACH, ring, lanes)
        p_ext[m, :, own_planes, rows:ring, :] = product(y_pieces, m).reshape(
            halves, depth, ring - rows, lanes
        )

    def first(m, carry):
        shift = table_ref[index_ref[m]]
        a, c = zero, zero
        for z in range(-1, depth + 1):
            image = apply(
                lambda k: [p_ext[m, h, k + REACH] for h in range(halves)], z, shift
            )
            for h in range(halves):
                value = image[h] * row_mask
                if z < 0:
                    value = value * present(-1, 0)
                elif z >= depth:
                    value = value * present(1, 0)
                else:
                    p = p_ext[m, h, z + REACH, 0:rows, :]
                    a = fold(a, p * r_ext[h, z + REACH, 0:rows, :])
                    c = fold(c, p * value[0:rows])
                q_ext[m, h, z + 1] = value
        put(0, m, a)
        put(1, m, c)
        return carry

    lax.fori_loop(0, systems, first, 0)

    a_own, c_own = coefs[0], coefs[1]
    sigma = jnp.where(a_own > 0.0, c_own / jnp.where(a_own > 0.0, a_own, 1.0), 0.0)
    coefs[5] = sigma

    def second(m, carry):
        shift = table_ref[index_ref[m]]
        s_row = coefs[5, pl.ds(m, 1), :]
        q_shifted = q_ext[m] - s_row[None, None] * r_ext[:, 1 : REACH + depth + 1]
        w_ext[m] = product(pieces(q_shifted), m).reshape(q_shifted.shape)
        g, f, e = zero, zero, zero
        for z in range(depth):
            image = apply(lambda k: [w_ext[m, h, k + 1] for h in range(halves)], z, shift)
            for h in range(halves):
                y = image[h][0:rows]
                w = w_ext[m, h, z + 1, 0:rows, :]
                q = q_ext[m, h, z + 1, 0:rows, :] - s_row * r_ext[h, z + REACH, 0:rows, :]
                g = fold(g, w * q)
                f = fold(f, p_ext[m, h, z + REACH, 0:rows, :] * y)
                e = fold(e, w * y)
                y_own[m, h, z] = y
        put(2, m, g)
        put(3, m, f)
        put(4, m, e)
        return carry

    lax.fori_loop(0, systems, second, 0)

    for r in range(rounds):
        pl.semaphore_wait(near_sem.at[r], near)
        if r + 1 < rounds:
            signal_near(near_sem.at[r + 1])

    lane = lax.broadcasted_iota(jnp.int32, (systems, lanes), 1)
    packed = coefs[0]
    for quantity in range(1, 6):
        packed = jnp.where(lane == quantity, coefs[quantity], packed)
    message[...] = packed
    gathered[me] = packed

    def gather_copy(device, source):
        return pltpu.make_async_remote_copy(
            src_ref=message,
            dst_ref=gathered.at[source],
            send_sem=gather_send_sem.at[source],
            recv_sem=gather_recv_sem.at[source],
            device_id=device,
            device_id_type=MESH,
        )

    def send_to(offset):
        peer, device = peer_of(offset)
        return pltpu.make_async_remote_copy(
            src_ref=message,
            dst_ref=gathered.at[me],
            send_sem=gather_send_sem.at[peer],
            recv_sem=gather_recv_sem.at[me],
            device_id=device,
            device_id_type=MESH,
        )

    def send_step(offset, carry):
        send_to(offset).start()
        return carry

    lax.fori_loop(1, group, send_step, 0)

    def receive_step(offset, carry):
        peer, device = peer_of(offset)
        gather_copy(device, peer).wait_recv()
        return carry

    lax.fori_loop(1, group, receive_step, 0)

    def column(source, quantity):
        return jnp.broadcast_to(
            gathered[source][:, quantity : quantity + 1], (systems, lanes)
        )

    a_all = [column(d, 0) for d in range(group)]
    c_all = [column(d, 1) for d in range(group)]
    rz_0, curvature_0 = sum(a_all), sum(c_all)
    alpha_0 = rz_0 / curvature_0
    kept = [1.0 - alpha_0 * column(d, 5) for d in range(group)]
    g_all = [column(d, 2) for d in range(group)]
    rz_1 = sum(
        kept[d] * kept[d] * a_all[d] + alpha_0 * alpha_0 * g_all[d] for d in range(group)
    )
    beta = rz_1 / rz_0
    curvature_1 = zero
    for d in range(group):
        k = kept[d] + beta
        curvature_1 = curvature_1 + (
            k * k * c_all[d]
            - alpha_0 * k * (column(d, 3) + g_all[d])
            + alpha_0 * alpha_0 * column(d, 4)
        )
    alpha_1 = rz_1 / curvature_1
    own_k = 1.0 - alpha_0 * sigma + beta
    coefs[0] = alpha_0 + alpha_1 * own_k
    coefs[1] = alpha_0 * alpha_1

    def close_send(offset, carry):
        send_to(offset).wait_send()
        return carry

    lax.fori_loop(1, group, close_send, 0)
    for dz, dy in DIRECTIONS:

        @pl.when(has(dz, dy))
        def _(dz=dz, dy=dy):
            label_copy(dz, dy).wait_send()
            halo_copy(dz, dy).wait_send()


def finish(
    r_ext, p_ext, q_ext, w_ext, y_own, coefs, solution_ref, residual_ref, out_s, out_r, out_sem
):
    systems, halves, depth, rows, lanes = y_own.shape
    own = slice(REACH, REACH + depth)
    copies = []
    for m in range(systems):
        main = coefs[0, m : m + 1, :][None]
        side = coefs[1, m : m + 1, :][None]
        for h in range(halves):
            cut = slice(h * lanes, (h + 1) * lanes)
            out_s[m, :, :, cut] = (
                main * p_ext[m, h, own, 0:rows, :] - side * w_ext[m, h, 1 : depth + 1, 0:rows, :]
            )
            out_r[m, :, :, cut] = (
                r_ext[h, own, 0:rows, :]
                - main * q_ext[m, h, 1 : depth + 1, 0:rows, :]
                + side * y_own[m, h]
            )
        for i, (source, target) in enumerate(((out_s, solution_ref), (out_r, residual_ref))):
            copies.append(pltpu.make_async_copy(source.at[m], target.at[m], out_sem.at[i, m]))
            copies[-1].start()
    for copy in copies:
        copy.wait()


def on_device(
    grid, right_side, labels, region_coeff, shift_index, shift_table, time_step, block_inverse
):
    depth, rows, nx = right_side.shape
    systems, lanes = block_inverse.shape[0], block_inverse.shape[1]
    halves = nx // lanes
    assert depth == EDGE and labels.shape[0] == 1
    group = grid[0] * grid[1]
    ring = rows + EDGE
    y_blocks = labels.shape[1]
    label_pad = -(-9 * y_blocks // 8) * 8
    f32 = jnp.float32
    vmem = pl.BlockSpec(memory_space=pltpu.VMEM)
    hbm = pl.BlockSpec(memory_space=pltpu.HBM)
    out = jax.ShapeDtypeStruct((systems,) + right_side.shape, f32)
    dma = pltpu.SemaphoreType.DMA
    tall, wide = depth + 2 * REACH, depth + 2
    fields = pl.pallas_call(
        functools.partial(kernel, grid),
        out_shape=tuple(
            jax.ShapeDtypeStruct(shape, f32)
            for shape in (
                (halves, tall, ring, lanes),
                (systems, halves, tall, ring, lanes),
                (systems, halves, wide, ring, lanes),
                (systems, halves, wide, ring, lanes),
                (systems, halves, depth, rows, lanes),
                (6, systems, lanes),
            )
        ),
        in_specs=[hbm] * 7,
        out_specs=(vmem,) * 6,
        scratch_shapes=[
            pltpu.VMEM(right_side.shape, f32),
            pltpu.VMEM(labels.shape, jnp.int32),
            pltpu.SMEM(region_coeff.shape, f32),
            pltpu.SMEM(shift_index.shape, jnp.int32),
            pltpu.SMEM(shift_table.shape, f32),
            pltpu.SMEM(time_step.shape, f32),
            pltpu.VMEM(block_inverse.shape, f32),
            pltpu.VMEM((systems, 2 * lanes, 2 * lanes), jnp.bfloat16),
            pltpu.VMEM((label_pad, nx), f32),
            pltpu.VMEM((label_pad, labels.shape[2]), f32),
            pltpu.VMEM((3, halves, ring, lanes), f32),
            pltpu.VMEM((5, halves, ring, lanes), f32),
            pltpu.VMEM((2, depth, REACH, nx), f32),
            pltpu.VMEM((2, REACH, rows, nx), f32),
            pltpu.VMEM((2, depth, REACH, nx), f32),
            pltpu.VMEM((2, 2, REACH, REACH, nx), f32),
            pltpu.VMEM((9,) + labels.shape, jnp.int32),
            pltpu.VMEM((systems, lanes), f32),
            pltpu.VMEM((group, systems, lanes), f32),
            dma((7,)),
            pltpu.SemaphoreType.REGULAR((max(1, max(grid) - 3),)),
            dma((9,)),
            dma((9,)),
            dma((9,)),
            dma((9,)),
            dma((group,)),
            dma((group,)),
        ],
        compiler_params=pltpu.CompilerParams(
            collective_id=0, has_side_effects=True, vmem_limit_bytes=32 * 1024 * 1024
        ),
    )(right_side, labels, region_coeff, shift_index, shift_table, time_step, block_inverse)
    return pl.pallas_call(
        finish,
        out_shape=(out, out),
        in_specs=[vmem] * 6,
        out_specs=(hbm, hbm),
        scratch_shapes=[pltpu.VMEM(out.shape, f32), pltpu.VMEM(out.shape, f32), dma((2, systems))],
        compiler_params=pltpu.CompilerParams(vmem_limit_bytes=32 * 1024 * 1024),
    )(*fields)


def solution(mesh):
    in_specs = (
        P(("sample", "gz"), "gy", None),
        P(("sample", "gz"), "gy", None),
        P("sample"),
        P("sample"),
        P(),
        P("sample"),
        P(),
    )
    out_specs = (P(None, ("sample", "gz"), "gy", None), P(None, ("sample", "gz"), "gy", None))
    grid = (mesh.shape["gz"], mesh.shape["gy"])
    return jax.shard_map(
        functools.partial(on_device, grid),
        mesh=mesh,
        in_specs=in_specs,
        out_specs=out_specs,
        check_vma=False,
    )
```

```python
import functools

import jax
import jax.numpy as jnp
from jax import lax
from jax.experimental import pallas as pl
from jax.experimental.pallas import tpu as pltpu
from jax.sharding import PartitionSpec as P

MESH = pl.DeviceIdType.MESH
EDGE = 8
REACH = 2
DIRECTIONS = [(dz, dy) for dz in (-1, 0, 1) for dy in (-1, 0, 1) if (dz, dy) != (0, 0)]


def slot(dz, dy):
    return (dz + 1) * 3 + dy + 1


def split(x):
    high = x.astype(jnp.bfloat16)
    low = (x - high.astype(jnp.float32)).astype(jnp.bfloat16)
    return high, low


def smooth_x(parts):
    width = parts[0].shape[1]
    lane = lax.broadcasted_iota(jnp.int32, parts[0].shape, 1)
    first, last = lane == 0, lane == width - 1
    rolled = [pltpu.roll(u, 1, 1) for u in parts]
    pairs = [
        u + jnp.where(first, rolled[i - 1] if i else 0.0, rolled[i]) for i, u in enumerate(parts)
    ]
    rolled = [pltpu.roll(h, width - 1, 1) for h in pairs]
    return [
        h + jnp.where(last, rolled[i + 1] if i + 1 < len(pairs) else parts[i], rolled[i])
        for i, h in enumerate(pairs)
    ]


def smooth_y(u):
    h = u + pltpu.roll(u, 1, 0)
    return h + pltpu.roll(h, u.shape[0] - 1, 0)


def smooth_xy(parts):
    return [smooth_y(u) for u in smooth_x(parts)]


def kernel(
    grid,
    right_hbm,
    labels_hbm,
    coeff_hbm,
    index_hbm,
    table_hbm,
    step_hbm,
    inverse_hbm,
    r_ext,
    p_ext,
    q_ext,
    w_ext,
    y_own,
    coefs,
    right_ref,
    labels_ref,
    coeff_ref,
    index_ref,
    table_ref,
    step_ref,
    inverse_ref,
    weights,
    c_rows,
    label_rows,
    c_planes,
    diag,
    y_send,
    z_recv,
    y_recv,
    corner_recv,
    label_recv,
    message,
    gathered,
    load_sem,
    near_sem,
    send_sem,
    recv_sem,
    label_send_sem,
    label_recv_sem,
    gather_send_sem,
    gather_recv_sem,
):
    n_gz, n_gy = grid
    group = n_gz * n_gy
    depth, rows, nx = right_ref.shape
    systems, lanes = inverse_ref.shape[0], inverse_ref.shape[1]
    halves = nx // lanes
    ring = r_ext.shape[2]
    y_blocks = labels_ref.shape[1]
    label_cols = labels_ref.shape[2]
    sample, gz, gy = lax.axis_index("sample"), lax.axis_index("gz"), lax.axis_index("gy")
    me = gz * n_gy + gy

    def has(dz, dy):
        z_ok = gz + dz >= 0 if dz < 0 else gz + dz < n_gz
        y_ok = gy + dy >= 0 if dy < 0 else gy + dy < n_gy
        return jnp.logical_and(z_ok, y_ok)

    def present(dz, dy):
        return jnp.where(has(dz, dy), 1.0, 0.0).astype(jnp.float32)

    def peer_of(offset):
        peer = lax.rem(me + offset, group)
        return peer, (sample, lax.div(peer, n_gy), lax.rem(peer, n_gy))

    loads = [
        pltpu.make_async_copy(source, target, load_sem.at[i])
        for i, (source, target) in enumerate(
            (
                (right_hbm, right_ref),
                (labels_hbm, labels_ref),
                (inverse_hbm, inverse_ref),
                (coeff_hbm, coeff_ref),
                (step_hbm, step_ref),
                (index_hbm, index_ref),
                (table_hbm, table_ref),
            )
        )
    ]
    for load in loads:
        load.start()

    z_recv[...] = jnp.zeros_like(z_recv)
    y_recv[...] = jnp.zeros_like(y_recv)
    corner_recv[...] = jnp.zeros_like(corner_recv)
    label_recv[...] = jnp.zeros_like(label_recv)

    barrier = pltpu.get_barrier_semaphore()

    def signal_near(semaphore):
        for dz, dy in DIRECTIONS:

            @pl.when(has(dz, dy))
            def _(dz=dz, dy=dy):
                pl.semaphore_signal(
                    semaphore,
                    inc=1,
                    device_id=(sample, gz + dz, gy + dy),
                    device_id_type=MESH,
                )

    z_near = 1 + (gz > 0).astype(jnp.int32) + (gz < n_gz - 1).astype(jnp.int32)
    y_near = 1 + (gy > 0).astype(jnp.int32) + (gy < n_gy - 1).astype(jnp.int32)
    near = z_near * y_near - 1

    signal_near(barrier)
    r_ext[...] = jnp.zeros_like(r_ext)
    loads[0].wait()
    loads[1].wait()
    y_send[0] = right_ref[:, 0:REACH, :]
    y_send[1] = right_ref[:, rows - REACH : rows, :]
    for h in range(halves):
        r_ext[h, REACH : REACH + depth, 0:rows, :] = right_ref[:, :, h * lanes : (h + 1) * lanes]

    pl.semaphore_wait(barrier, near)

    def halo_copy(dz, dy):
        device = (sample, gz + dz, gy + dy)
        z_from = depth - REACH if dz > 0 else 0
        if dy == 0:
            source = right_ref.at[pl.ds(z_from, REACH)]
            target = z_recv.at[0 if dz > 0 else 1]
        elif dz == 0:
            source = y_send.at[1 if dy > 0 else 0]
            target = y_recv.at[0 if dy > 0 else 1]
        else:
            source = y_send.at[1 if dy > 0 else 0, pl.ds(z_from, REACH)]
            target = corner_recv.at[0 if dz > 0 else 1, 0 if dy > 0 else 1]
        return pltpu.make_async_remote_copy(
            src_ref=source,
            dst_ref=target,
            send_sem=send_sem.at[slot(dz, dy)],
            recv_sem=recv_sem.at[slot(-dz, -dy)],
            device_id=device,
            device_id_type=MESH,
        )

    def label_copy(dz, dy):
        return pltpu.make_async_remote_copy(
            src_ref=labels_ref,
            dst_ref=label_recv.at[slot(-dz, -dy)],
            send_sem=label_send_sem.at[slot(dz, dy)],
            recv_sem=label_recv_sem.at[slot(-dz, -dy)],
            device_id=(sample, gz + dz, gy + dy),
            device_id_type=MESH,
        )

    for dz, dy in DIRECTIONS:

        @pl.when(has(dz, dy))
        def _(dz=dz, dy=dy):
            label_copy(dz, dy).start()
            halo_copy(dz, dy).start()

    for load in loads[2:]:
        load.wait()
    for m in range(systems):
        high, low = split(inverse_ref[m])
        weights[m, 0:lanes, 0:lanes] = high
        weights[m, lanes : 2 * lanes, 0:lanes] = high
        weights[m, 0:lanes, lanes : 2 * lanes] = low
        weights[m, lanes : 2 * lanes, lanes : 2 * lanes] = low

    def pieces(x):
        return jnp.concatenate(split(x.reshape(-1, lanes)), axis=1)

    def product(x, m):
        both = jnp.dot(x, weights[m], preferred_element_type=jnp.float32)
        return both[:, 0:lanes] + both[:, lanes : 2 * lanes]

    own_planes = slice(REACH, REACH + depth)
    own_pieces = pieces(r_ext[:, own_planes, 0:rows, :])
    for m in range(systems):
        p_ext[m, :, own_planes, 0:rows, :] = product(own_pieces, m).reshape(
            halves, depth, rows, lanes
        )

    for dz, dy in DIRECTIONS:

        @pl.when(has(dz, dy))
        def _(dz=dz, dy=dy):
            label_copy(-dz, -dy).wait_recv()
            halo_copy(-dz, -dy).wait_recv()

    rounds = max(n_gz, n_gy) - 3
    if rounds > 0:
        signal_near(near_sem.at[0])

    for h in range(halves):
        cut = slice(h * lanes, (h + 1) * lanes)
        for side in (0, 1):
            planes = slice(0, REACH) if side == 0 else slice(REACH + depth, 2 * REACH + depth)
            r_ext[h, planes, 0:rows, :] = z_recv[side, :, :, cut]
            r_ext[h, planes, rows : rows + REACH, :] = corner_recv[side, 1, :, :, cut]
            r_ext[h, planes, ring - REACH : ring, :] = corner_recv[side, 0, :, :, cut]
        own = slice(REACH, REACH + depth)
        r_ext[h, own, rows : rows + REACH, :] = y_recv[1, :, :, cut]
        r_ext[h, own, ring - REACH : ring, :] = y_recv[0, :, :, cut]

    label_rows[...] = jnp.zeros_like(label_rows)
    for s in range(9):
        table = labels_ref[0] if s == slot(0, 0) else label_recv[s, 0]
        label_rows[s * y_blocks : (s + 1) * y_blocks, :] = table.astype(jnp.float32)
    spread = jnp.where(
        lax.broadcasted_iota(jnp.int32, (label_cols, nx), 0)
        == lax.broadcasted_iota(jnp.int32, (label_cols, nx), 1) // EDGE,
        1.0,
        0.0,
    ).astype(jnp.bfloat16)
    wide = jnp.dot(
        label_rows[...].astype(jnp.bfloat16), spread, preferred_element_type=jnp.float32
    )
    cells = jnp.zeros_like(wide)
    scale = step_ref[0] * 0.125
    for region in range(coeff_ref.shape[0]):
        cells = jnp.where(wide == float(region), coeff_ref[region] * scale, cells)
    c_rows[...] = cells

    sub = lax.broadcasted_iota(jnp.int32, (EDGE, lanes), 0)
    for dz in (-1, 0, 1):
        for h in range(halves):
            cut = slice(h * lanes, (h + 1) * lanes)

            def row(dy, block):
                at = slot(dz, dy) * y_blocks + block
                value = c_rows[at : at + 1, cut]
                if (dz, dy) != (0, 0):
                    value = value * present(dz, dy)
                return jnp.broadcast_to(value, (EDGE, lanes))

            for block in range(y_blocks):
                c_planes[dz + 1, h, block * EDGE : (block + 1) * EDGE, :] = row(0, block)
            c_planes[dz + 1, h, rows:ring, :] = jnp.where(
                sub < EDGE // 2, row(1, 0), row(-1, y_blocks - 1)
            )

    smooth = [smooth_xy([c_planes[d, h] for h in range(halves)]) for d in range(3)]
    for h in range(halves):
        low, own, high = (smooth[d][h] for d in range(3))
        diag[0, h] = 3.0 * low + own + 64.0 * c_planes[0, h]
        diag[1, h] = low + 3.0 * own + 64.0 * c_planes[1, h]
        diag[2, h] = 4.0 * own + 64.0 * c_planes[1, h]
        diag[3, h] = high + 3.0 * own + 64.0 * c_planes[1, h]
        diag[4, h] = 3.0 * high + own + 64.0 * c_planes[2, h]

    ring_row = lax.broadcasted_iota(jnp.int32, (ring, lanes), 0)
    row_mask = jnp.where(
        ring_row < rows,
        1.0,
        jnp.where(ring_row < rows + EDGE // 2, present(0, 1), present(0, -1)),
    )

    def apply(field, z, shift):
        def c_of(plane):
            return 0 if plane < 0 else 2 if plane >= depth else 1

        below, here, above = field(z - 1), field(z), field(z + 1)
        kind = 0 if z < 0 else 4 if z >= depth else 1 if z == 0 else 3 if z == depth - 1 else 2
        ku, kcu = [], []
        for h in range(halves):
            u = (below[h] + here[h]) + (here[h] + above[h])
            if kind == 2:
                cu = c_planes[1, h] * u
            else:
                cu = (
                    c_planes[c_of(z - 1), h] * below[h]
                    + 2.0 * (c_planes[c_of(z), h] * here[h])
                    + c_planes[c_of(z + 1), h] * above[h]
                )
            ku.append(u)
            kcu.append(cu)
        ku, kcu = smooth_xy(ku), smooth_xy(kcu)
        return [
            (diag[kind, h] + shift) * here[h] - c_planes[c_of(z), h] * ku[h] - kcu[h]
            for h in range(halves)
        ]

    def fold(total, term):
        term = term.reshape(-1, 8, lanes)
        for i in range(term.shape[0]):
            total = total + term[i]
        return total

    def put(quantity, m, total):
        value = jnp.sum(jnp.sum(total, axis=0, keepdims=True), axis=1, keepdims=True)
        coefs[quantity, pl.ds(m, 1), :] = jnp.broadcast_to(value, (1, lanes))

    zero = jnp.zeros((8, lanes), jnp.float32)

    z_pieces = [
        pieces(r_ext[:, planes])
        for planes in (slice(0, REACH), slice(REACH + depth, 2 * REACH + depth))
    ]
    y_pieces = pieces(r_ext[:, own_planes, rows:ring, :])
    for m in range(systems):
        for planes, x in zip(
            (slice(0, REACH), slice(REACH + depth, 2 * REACH + depth)), z_pieces
        ):
            p_ext[m, :, planes] = product(x, m).reshape(halves, REACH, ring, lanes)
        p_ext[m, :, own_planes, rows:ring, :] = product(y_pieces, m).reshape(
            halves, depth, ring - rows, lanes
        )

    def first(m, carry):
        shift = table_ref[index_ref[m]]
        a, c = zero, zero
        for z in range(-1, depth + 1):
            image = apply(
                lambda k: [p_ext[m, h, k + REACH] for h in range(halves)], z, shift
            )
            for h in range(halves):
                value = image[h] * row_mask
                if z < 0:
                    value = value * present(-1, 0)
                elif z >= depth:
                    value = value * present(1, 0)
                else:
                    p = p_ext[m, h, z + REACH, 0:rows, :]
                    a = fold(a, p * r_ext[h, z + REACH, 0:rows, :])
                    c = fold(c, p * value[0:rows])
                q_ext[m, h, z + 1] = value
        put(0, m, a)
        put(1, m, c)
        return carry

    lax.fori_loop(0, systems, first, 0)

    a_own, c_own = coefs[0], coefs[1]
    sigma = jnp.where(a_own > 0.0, c_own / jnp.where(a_own > 0.0, a_own, 1.0), 0.0)
    coefs[5] = sigma

    def second(m, carry):
        shift = table_ref[index_ref[m]]
        s_row = coefs[5, pl.ds(m, 1), :]
        q_shifted = q_ext[m] - s_row[None, None] * r_ext[:, 1 : REACH + depth + 1]
        w_ext[m] = product(pieces(q_shifted), m).reshape(q_shifted.shape)
        g, f, e = zero, zero, zero
        for z in range(depth):
            image = apply(lambda k: [w_ext[m, h, k + 1] for h in range(halves)], z, shift)
            for h in range(halves):
                y = image[h][0:rows]
                w = w_ext[m, h, z + 1, 0:rows, :]
                q = q_ext[m, h, z + 1, 0:rows, :] - s_row * r_ext[h, z + REACH, 0:rows, :]
                g = fold(g, w * q)
                f = fold(f, p_ext[m, h, z + REACH, 0:rows, :] * y)
                e = fold(e, w * y)
                y_own[m, h, z] = y
        put(2, m, g)
        put(3, m, f)
        put(4, m, e)
        return carry

    lax.fori_loop(0, systems, second, 0)

    for r in range(rounds):
        pl.semaphore_wait(near_sem.at[r], near)
        if r + 1 < rounds:
            signal_near(near_sem.at[r + 1])

    lane = lax.broadcasted_iota(jnp.int32, (systems, lanes), 1)
    packed = coefs[0]
    for quantity in range(1, 6):
        packed = jnp.where(lane == quantity, coefs[quantity], packed)
    message[...] = packed
    gathered[me] = packed

    def gather_copy(device, source):
        return pltpu.make_async_remote_copy(
            src_ref=message,
            dst_ref=gathered.at[source],
            send_sem=gather_send_sem.at[source],
            recv_sem=gather_recv_sem.at[source],
            device_id=device,
            device_id_type=MESH,
        )

    def send_to(offset):
        peer, device = peer_of(offset)
        return pltpu.make_async_remote_copy(
            src_ref=message,
            dst_ref=gathered.at[me],
            send_sem=gather_send_sem.at[peer],
            recv_sem=gather_recv_sem.at[me],
            device_id=device,
            device_id_type=MESH,
        )

    def send_step(offset, carry):
        send_to(offset).start()
        return carry

    lax.fori_loop(1, group, send_step, 0)

    def receive_step(offset, carry):
        peer, device = peer_of(offset)
        gather_copy(device, peer).wait_recv()
        return carry

    lax.fori_loop(1, group, receive_step, 0)

    def column(source, quantity):
        return jnp.broadcast_to(
            gathered[source][:, quantity : quantity + 1], (systems, lanes)
        )

    a_all = [column(d, 0) for d in range(group)]
    c_all = [column(d, 1) for d in range(group)]
    rz_0, curvature_0 = sum(a_all), sum(c_all)
    alpha_0 = rz_0 / curvature_0
    kept = [1.0 - alpha_0 * column(d, 5) for d in range(group)]
    g_all = [column(d, 2) for d in range(group)]
    rz_1 = sum(
        kept[d] * kept[d] * a_all[d] + alpha_0 * alpha_0 * g_all[d] for d in range(group)
    )
    beta = rz_1 / rz_0
    curvature_1 = zero
    for d in range(group):
        k = kept[d] + beta
        curvature_1 = curvature_1 + (
            k * k * c_all[d]
            - alpha_0 * k * (column(d, 3) + g_all[d])
            + alpha_0 * alpha_0 * column(d, 4)
        )
    alpha_1 = rz_1 / curvature_1
    own_k = 1.0 - alpha_0 * sigma + beta
    coefs[0] = alpha_0 + alpha_1 * own_k
    coefs[1] = alpha_0 * alpha_1

    def close_send(offset, carry):
        send_to(offset).wait_send()
        return carry

    lax.fori_loop(1, group, close_send, 0)
    for dz, dy in DIRECTIONS:

        @pl.when(has(dz, dy))
        def _(dz=dz, dy=dy):
            label_copy(dz, dy).wait_send()
            halo_copy(dz, dy).wait_send()


def finish(
    r_ext, p_ext, q_ext, w_ext, y_own, coefs, solution_ref, residual_ref, out_s, out_r, out_sem
):
    systems, halves, depth, rows, lanes = y_own.shape
    own = slice(REACH, REACH + depth)
    copies = []
    for m in range(systems):
        main = coefs[0, m : m + 1, :][None]
        side = coefs[1, m : m + 1, :][None]
        for h in range(halves):
            cut = slice(h * lanes, (h + 1) * lanes)
            out_s[m, :, :, cut] = (
                main * p_ext[m, h, own, 0:rows, :] - side * w_ext[m, h, 1 : depth + 1, 0:rows, :]
            )
            out_r[m, :, :, cut] = (
                r_ext[h, own, 0:rows, :]
                - main * q_ext[m, h, 1 : depth + 1, 0:rows, :]
                + side * y_own[m, h]
            )
        for i, (source, target) in enumerate(((out_s, solution_ref), (out_r, residual_ref))):
            copies.append(pltpu.make_async_copy(source.at[m], target.at[m], out_sem.at[i, m]))
            copies[-1].start()
    for copy in copies:
        copy.wait()


def on_device(
    grid, right_side, labels, region_coeff, shift_index, shift_table, time_step, block_inverse
):
    depth, rows, nx = right_side.shape
    systems, lanes = block_inverse.shape[0], block_inverse.shape[1]
    halves = nx // lanes
    assert depth == EDGE and labels.shape[0] == 1
    group = grid[0] * grid[1]
    ring = rows + EDGE
    y_blocks = labels.shape[1]
    label_pad = -(-9 * y_blocks // 8) * 8
    f32 = jnp.float32
    vmem = pl.BlockSpec(memory_space=pltpu.VMEM)
    hbm = pl.BlockSpec(memory_space=pltpu.HBM)
    out = jax.ShapeDtypeStruct((systems,) + right_side.shape, f32)
    dma = pltpu.SemaphoreType.DMA
    tall, wide = depth + 2 * REACH, depth + 2
    fields = pl.pallas_call(
        functools.partial(kernel, grid),
        out_shape=tuple(
            jax.ShapeDtypeStruct(shape, f32)
            for shape in (
                (halves, tall, ring, lanes),
                (systems, halves, tall, ring, lanes),
                (systems, halves, wide, ring, lanes),
                (systems, halves, wide, ring, lanes),
                (systems, halves, depth, rows, lanes),
                (6, systems, lanes),
            )
        ),
        in_specs=[hbm] * 7,
        out_specs=(vmem,) * 6,
        scratch_shapes=[
            pltpu.VMEM(right_side.shape, f32),
            pltpu.VMEM(labels.shape, jnp.int32),
            pltpu.SMEM(region_coeff.shape, f32),
            pltpu.SMEM(shift_index.shape, jnp.int32),
            pltpu.SMEM(shift_table.shape, f32),
            pltpu.SMEM(time_step.shape, f32),
            pltpu.VMEM(block_inverse.shape, f32),
            pltpu.VMEM((systems, 2 * lanes, 2 * lanes), jnp.bfloat16),
            pltpu.VMEM((label_pad, nx), f32),
            pltpu.VMEM((label_pad, labels.shape[2]), f32),
            pltpu.VMEM((3, halves, ring, lanes), f32),
            pltpu.VMEM((5, halves, ring, lanes), f32),
            pltpu.VMEM((2, depth, REACH, nx), f32),
            pltpu.VMEM((2, REACH, rows, nx), f32),
            pltpu.VMEM((2, depth, REACH, nx), f32),
            pltpu.VMEM((2, 2, REACH, REACH, nx), f32),
            pltpu.VMEM((9,) + labels.shape, jnp.int32),
            pltpu.VMEM((systems, lanes), f32),
            pltpu.VMEM((group, systems, lanes), f32),
            dma((7,)),
            pltpu.SemaphoreType.REGULAR((max(1, max(grid) - 3),)),
            dma((9,)),
            dma((9,)),
            dma((9,)),
            dma((9,)),
            dma((group,)),
            dma((group,)),
        ],
        compiler_params=pltpu.CompilerParams(
            collective_id=0, has_side_effects=True, vmem_limit_bytes=32 * 1024 * 1024
        ),
    )(
        *(
            x if x is time_step else pltpu.with_memory_space_constraint(x, pltpu.HBM)
            for x in (
                right_side,
                labels,
                region_coeff,
                shift_index,
                shift_table,
                time_step,
                block_inverse,
            )
        )
    )
    return pl.pallas_call(
        finish,
        out_shape=(out, out),
        in_specs=[vmem] * 6,
        out_specs=(hbm, hbm),
        scratch_shapes=[pltpu.VMEM(out.shape, f32), pltpu.VMEM(out.shape, f32), dma((2, systems))],
        compiler_params=pltpu.CompilerParams(vmem_limit_bytes=32 * 1024 * 1024),
    )(*fields)


def solution(mesh):
    in_specs = (
        P(("sample", "gz"), "gy", None),
        P(("sample", "gz"), "gy", None),
        P("sample"),
        P("sample"),
        P(),
        P("sample"),
        P(),
    )
    out_specs = (P(None, ("sample", "gz"), "gy", None), P(None, ("sample", "gz"), "gy", None))
    grid = (mesh.shape["gz"], mesh.shape["gy"])
    return jax.shard_map(
        functools.partial(on_device, grid),
        mesh=mesh,
        in_specs=in_specs,
        out_specs=out_specs,
        check_vma=False,
    )
```

```python
import functools

import jax
import jax.numpy as jnp
from jax import lax
from jax.experimental import pallas as pl
from jax.experimental.pallas import tpu as pltpu
from jax.sharding import PartitionSpec as P

MESH = pl.DeviceIdType.MESH
EDGE = 8
REACH = 2
DIRECTIONS = [(dz, dy) for dz in (-1, 0, 1) for dy in (-1, 0, 1) if (dz, dy) != (0, 0)]


def slot(dz, dy):
    return (dz + 1) * 3 + dy + 1


def split(x):
    high = x.astype(jnp.bfloat16)
    low = (x - high.astype(jnp.float32)).astype(jnp.bfloat16)
    return high, low


def smooth_x(parts):
    width = parts[0].shape[1]
    lane = lax.broadcasted_iota(jnp.int32, parts[0].shape, 1)
    first, last = lane == 0, lane == width - 1
    rolled = [pltpu.roll(u, 1, 1) for u in parts]
    pairs = [
        u + jnp.where(first, rolled[i - 1] if i else 0.0, rolled[i]) for i, u in enumerate(parts)
    ]
    rolled = [pltpu.roll(h, width - 1, 1) for h in pairs]
    return [
        h + jnp.where(last, rolled[i + 1] if i + 1 < len(pairs) else parts[i], rolled[i])
        for i, h in enumerate(pairs)
    ]


def smooth_y(u):
    h = u + pltpu.roll(u, 1, 0)
    return h + pltpu.roll(h, u.shape[0] - 1, 0)


def smooth_xy(parts):
    return [smooth_y(u) for u in smooth_x(parts)]


def kernel(
    grid,
    right_hbm,
    labels_hbm,
    coeff_hbm,
    index_hbm,
    table_hbm,
    step_hbm,
    inverse_hbm,
    r_ext,
    p_ext,
    q_ext,
    w_ext,
    y_own,
    coefs,
    right_ref,
    labels_ref,
    coeff_ref,
    index_ref,
    table_ref,
    step_ref,
    inverse_ref,
    weights,
    c_rows,
    label_rows,
    c_planes,
    diag,
    y_send,
    z_recv,
    y_recv,
    corner_recv,
    label_recv,
    message,
    gathered,
    table,
    load_sem,
    near_sem,
    send_sem,
    recv_sem,
    label_send_sem,
    label_recv_sem,
    gather_send_sem,
    gather_recv_sem,
):
    n_gz, n_gy = grid
    group = n_gz * n_gy
    depth, rows, nx = right_ref.shape
    systems, lanes = inverse_ref.shape[0], inverse_ref.shape[1]
    halves = nx // lanes
    ring = r_ext.shape[2]
    y_blocks = labels_ref.shape[1]
    label_cols = labels_ref.shape[2]
    sample, gz, gy = lax.axis_index("sample"), lax.axis_index("gz"), lax.axis_index("gy")
    me = gz * n_gy + gy

    def has(dz, dy):
        z_ok = gz + dz >= 0 if dz < 0 else gz + dz < n_gz
        y_ok = gy + dy >= 0 if dy < 0 else gy + dy < n_gy
        return jnp.logical_and(z_ok, y_ok)

    def present(dz, dy):
        return jnp.where(has(dz, dy), 1.0, 0.0).astype(jnp.float32)

    def peer_of(offset):
        peer = lax.rem(me + offset, group)
        return peer, (sample, lax.div(peer, n_gy), lax.rem(peer, n_gy))

    loads = [
        pltpu.make_async_copy(source, target, load_sem.at[i])
        for i, (source, target) in enumerate(
            (
                (right_hbm, right_ref),
                (labels_hbm, labels_ref),
                (inverse_hbm, inverse_ref),
                (coeff_hbm, coeff_ref),
                (step_hbm, step_ref),
                (index_hbm, index_ref),
                (table_hbm, table_ref),
            )
        )
    ]
    for load in loads:
        load.start()

    z_recv[...] = jnp.zeros_like(z_recv)
    y_recv[...] = jnp.zeros_like(y_recv)
    corner_recv[...] = jnp.zeros_like(corner_recv)
    label_recv[...] = jnp.zeros_like(label_recv)

    barrier = pltpu.get_barrier_semaphore()

    def signal_near(semaphore):
        for dz, dy in DIRECTIONS:

            @pl.when(has(dz, dy))
            def _(dz=dz, dy=dy):
                pl.semaphore_signal(
                    semaphore,
                    inc=1,
                    device_id=(sample, gz + dz, gy + dy),
                    device_id_type=MESH,
                )

    z_near = 1 + (gz > 0).astype(jnp.int32) + (gz < n_gz - 1).astype(jnp.int32)
    y_near = 1 + (gy > 0).astype(jnp.int32) + (gy < n_gy - 1).astype(jnp.int32)
    near = z_near * y_near - 1

    signal_near(barrier)
    r_ext[...] = jnp.zeros_like(r_ext)
    loads[0].wait()
    loads[1].wait()
    y_send[0] = right_ref[:, 0:REACH, :]
    y_send[1] = right_ref[:, rows - REACH : rows, :]
    for h in range(halves):
        r_ext[h, REACH : REACH + depth, 0:rows, :] = right_ref[:, :, h * lanes : (h + 1) * lanes]

    pl.semaphore_wait(barrier, near)

    def halo_copy(dz, dy):
        device = (sample, gz + dz, gy + dy)
        z_from = depth - REACH if dz > 0 else 0
        if dy == 0:
            source = right_ref.at[pl.ds(z_from, REACH)]
            target = z_recv.at[0 if dz > 0 else 1]
        elif dz == 0:
            source = y_send.at[1 if dy > 0 else 0]
            target = y_recv.at[0 if dy > 0 else 1]
        else:
            source = y_send.at[1 if dy > 0 else 0, pl.ds(z_from, REACH)]
            target = corner_recv.at[0 if dz > 0 else 1, 0 if dy > 0 else 1]
        return pltpu.make_async_remote_copy(
            src_ref=source,
            dst_ref=target,
            send_sem=send_sem.at[slot(dz, dy)],
            recv_sem=recv_sem.at[slot(-dz, -dy)],
            device_id=device,
            device_id_type=MESH,
        )

    def label_copy(dz, dy):
        return pltpu.make_async_remote_copy(
            src_ref=labels_ref,
            dst_ref=label_recv.at[slot(-dz, -dy)],
            send_sem=label_send_sem.at[slot(dz, dy)],
            recv_sem=label_recv_sem.at[slot(-dz, -dy)],
            device_id=(sample, gz + dz, gy + dy),
            device_id_type=MESH,
        )

    for dz, dy in DIRECTIONS:

        @pl.when(has(dz, dy))
        def _(dz=dz, dy=dy):
            label_copy(dz, dy).start()
            halo_copy(dz, dy).start()

    for load in loads[2:]:
        load.wait()
    for m in range(systems):
        high, low = split(inverse_ref[m])
        weights[m, 0:lanes, 0:lanes] = high
        weights[m, lanes : 2 * lanes, 0:lanes] = high
        weights[m, 0:lanes, lanes : 2 * lanes] = low
        weights[m, lanes : 2 * lanes, lanes : 2 * lanes] = low

    def pieces(x):
        return jnp.concatenate(split(x.reshape(-1, lanes)), axis=1)

    def product(x, m):
        both = jnp.dot(x, weights[m], preferred_element_type=jnp.float32)
        return both[:, 0:lanes] + both[:, lanes : 2 * lanes]

    own_planes = slice(REACH, REACH + depth)
    own_pieces = pieces(r_ext[:, own_planes, 0:rows, :])
    for m in range(systems):
        p_ext[m, :, own_planes, 0:rows, :] = product(own_pieces, m).reshape(
            halves, depth, rows, lanes
        )

    for dz, dy in DIRECTIONS:

        @pl.when(has(dz, dy))
        def _(dz=dz, dy=dy):
            label_copy(-dz, -dy).wait_recv()
            halo_copy(-dz, -dy).wait_recv()

    rounds = max(n_gz, n_gy) - 3
    if rounds > 0:
        signal_near(near_sem.at[0])

    for h in range(halves):
        cut = slice(h * lanes, (h + 1) * lanes)
        for side in (0, 1):
            planes = slice(0, REACH) if side == 0 else slice(REACH + depth, 2 * REACH + depth)
            r_ext[h, planes, 0:rows, :] = z_recv[side, :, :, cut]
            r_ext[h, planes, rows : rows + REACH, :] = corner_recv[side, 1, :, :, cut]
            r_ext[h, planes, ring - REACH : ring, :] = corner_recv[side, 0, :, :, cut]
        own = slice(REACH, REACH + depth)
        r_ext[h, own, rows : rows + REACH, :] = y_recv[1, :, :, cut]
        r_ext[h, own, ring - REACH : ring, :] = y_recv[0, :, :, cut]

    label_rows[...] = jnp.zeros_like(label_rows)
    for s in range(9):
        near_labels = labels_ref[0] if s == slot(0, 0) else label_recv[s, 0]
        label_rows[s * y_blocks : (s + 1) * y_blocks, :] = near_labels.astype(jnp.float32)
    spread = jnp.where(
        lax.broadcasted_iota(jnp.int32, (label_cols, nx), 0)
        == lax.broadcasted_iota(jnp.int32, (label_cols, nx), 1) // EDGE,
        1.0,
        0.0,
    ).astype(jnp.bfloat16)
    wide = jnp.dot(
        label_rows[...].astype(jnp.bfloat16), spread, preferred_element_type=jnp.float32
    )
    cells = jnp.zeros_like(wide)
    scale = step_ref[0] * 0.125
    for region in range(coeff_ref.shape[0]):
        cells = jnp.where(wide == float(region), coeff_ref[region] * scale, cells)
    c_rows[...] = cells

    sub = lax.broadcasted_iota(jnp.int32, (EDGE, lanes), 0)
    for dz in (-1, 0, 1):
        for h in range(halves):
            cut = slice(h * lanes, (h + 1) * lanes)

            def row(dy, block):
                at = slot(dz, dy) * y_blocks + block
                value = c_rows[at : at + 1, cut]
                if (dz, dy) != (0, 0):
                    value = value * present(dz, dy)
                return jnp.broadcast_to(value, (EDGE, lanes))

            for block in range(y_blocks):
                c_planes[dz + 1, h, block * EDGE : (block + 1) * EDGE, :] = row(0, block)
            c_planes[dz + 1, h, rows:ring, :] = jnp.where(
                sub < EDGE // 2, row(1, 0), row(-1, y_blocks - 1)
            )

    smooth = [smooth_xy([c_planes[d, h] for h in range(halves)]) for d in range(3)]
    for h in range(halves):
        low, own, high = (smooth[d][h] for d in range(3))
        diag[0, h] = 3.0 * low + own + 64.0 * c_planes[0, h]
        diag[1, h] = low + 3.0 * own + 64.0 * c_planes[1, h]
        diag[2, h] = 4.0 * own + 64.0 * c_planes[1, h]
        diag[3, h] = high + 3.0 * own + 64.0 * c_planes[1, h]
        diag[4, h] = 3.0 * high + own + 64.0 * c_planes[2, h]

    ring_row = lax.broadcasted_iota(jnp.int32, (ring, lanes), 0)
    row_mask = jnp.where(
        ring_row < rows,
        1.0,
        jnp.where(ring_row < rows + EDGE // 2, present(0, 1), present(0, -1)),
    )

    def apply(field, z, shift):
        def c_of(plane):
            return 0 if plane < 0 else 2 if plane >= depth else 1

        below, here, above = field(z - 1), field(z), field(z + 1)
        kind = 0 if z < 0 else 4 if z >= depth else 1 if z == 0 else 3 if z == depth - 1 else 2
        ku, kcu = [], []
        for h in range(halves):
            u = (below[h] + here[h]) + (here[h] + above[h])
            if kind == 2:
                cu = c_planes[1, h] * u
            else:
                cu = (
                    c_planes[c_of(z - 1), h] * below[h]
                    + 2.0 * (c_planes[c_of(z), h] * here[h])
                    + c_planes[c_of(z + 1), h] * above[h]
                )
            ku.append(u)
            kcu.append(cu)
        ku, kcu = smooth_xy(ku), smooth_xy(kcu)
        return [
            (diag[kind, h] + shift) * here[h] - c_planes[c_of(z), h] * ku[h] - kcu[h]
            for h in range(halves)
        ]

    def fold(total, term):
        term = term.reshape(-1, 8, lanes)
        for i in range(term.shape[0]):
            total = total + term[i]
        return total

    def put(quantity, m, total):
        value = jnp.sum(jnp.sum(total, axis=0, keepdims=True), axis=1, keepdims=True)
        coefs[quantity, pl.ds(m, 1), :] = jnp.broadcast_to(value, (1, lanes))

    zero = jnp.zeros((8, lanes), jnp.float32)

    z_pieces = [
        pieces(r_ext[:, planes])
        for planes in (slice(0, REACH), slice(REACH + depth, 2 * REACH + depth))
    ]
    y_pieces = pieces(r_ext[:, own_planes, rows:ring, :])
    for m in range(systems):
        for planes, x in zip(
            (slice(0, REACH), slice(REACH + depth, 2 * REACH + depth)), z_pieces
        ):
            p_ext[m, :, planes] = product(x, m).reshape(halves, REACH, ring, lanes)
        p_ext[m, :, own_planes, rows:ring, :] = product(y_pieces, m).reshape(
            halves, depth, ring - rows, lanes
        )

    def first(m, carry):
        shift = table_ref[index_ref[m]]
        a, c = zero, zero
        for z in range(-1, depth + 1):
            image = apply(
                lambda k: [p_ext[m, h, k + REACH] for h in range(halves)], z, shift
            )
            for h in range(halves):
                value = image[h] * row_mask
                if z < 0:
                    value = value * present(-1, 0)
                elif z >= depth:
                    value = value * present(1, 0)
                else:
                    p = p_ext[m, h, z + REACH, 0:rows, :]
                    a = fold(a, p * r_ext[h, z + REACH, 0:rows, :])
                    c = fold(c, p * value[0:rows])
                q_ext[m, h, z + 1] = value
        put(0, m, a)
        put(1, m, c)
        return carry

    lax.fori_loop(0, systems, first, 0)

    a_own, c_own = coefs[0], coefs[1]
    sigma = jnp.where(a_own > 0.0, c_own / jnp.where(a_own > 0.0, a_own, 1.0), 0.0)
    coefs[5] = sigma

    def second(m, carry):
        shift = table_ref[index_ref[m]]
        s_row = coefs[5, pl.ds(m, 1), :]
        q_shifted = q_ext[m] - s_row[None, None] * r_ext[:, 1 : REACH + depth + 1]
        w_ext[m] = product(pieces(q_shifted), m).reshape(q_shifted.shape)
        g, f, e = zero, zero, zero
        for z in range(depth):
            image = apply(lambda k: [w_ext[m, h, k + 1] for h in range(halves)], z, shift)
            for h in range(halves):
                y = image[h][0:rows]
                w = w_ext[m, h, z + 1, 0:rows, :]
                q = q_ext[m, h, z + 1, 0:rows, :] - s_row * r_ext[h, z + REACH, 0:rows, :]
                g = fold(g, w * q)
                f = fold(f, p_ext[m, h, z + REACH, 0:rows, :] * y)
                e = fold(e, w * y)
                y_own[m, h, z] = y
        put(2, m, g)
        put(3, m, f)
        put(4, m, e)
        return carry

    lax.fori_loop(0, systems, second, 0)

    for r in range(rounds):
        pl.semaphore_wait(near_sem.at[r], near)
        if r + 1 < rounds:
            signal_near(near_sem.at[r + 1])

    lane = lax.broadcasted_iota(jnp.int32, (systems, lanes), 1)
    place = lax.broadcasted_iota(jnp.int32, (systems, lanes), 0)
    packed = jnp.zeros((systems, lanes), jnp.float32)
    for quantity in range(6):
        packed = jnp.where(lane == place + quantity * systems, coefs[quantity], packed)
    packed = jnp.sum(packed, axis=0, keepdims=True)
    message[...] = packed

    def gather_copy(device, source):
        return pltpu.make_async_remote_copy(
            src_ref=message,
            dst_ref=gathered.at[source],
            send_sem=gather_send_sem.at[source],
            recv_sem=gather_recv_sem.at[source],
            device_id=device,
            device_id_type=MESH,
        )

    def send_to(offset):
        peer, device = peer_of(offset)
        return pltpu.make_async_remote_copy(
            src_ref=message,
            dst_ref=gathered.at[me],
            send_sem=gather_send_sem.at[peer],
            recv_sem=gather_recv_sem.at[me],
            device_id=device,
            device_id_type=MESH,
        )

    def send_step(offset, carry):
        send_to(offset).start()
        return carry

    lax.fori_loop(1, group, send_step, 0)

    def receive_step(offset, carry):
        peer, device = peer_of(offset)
        gather_copy(device, peer).wait_recv()
        return carry

    lax.fori_loop(1, group, receive_step, 0)

    gathered[me] = packed
    for source in range(group):
        table[source : source + 1, :] = gathered[source]

    def view(rows_of, quantity):
        return pltpu.roll(rows_of, lanes - quantity * systems, 1) if quantity else rows_of

    def over_devices(x):
        return jnp.sum(x, axis=0, keepdims=True)

    everyone = table[...]
    a_all, c_all, g_all, f_all, e_all, sigma_all = (view(everyone, i) for i in range(6))
    rz_0 = over_devices(a_all)
    alpha_0 = rz_0 / over_devices(c_all)
    kept = 1.0 - alpha_0 * sigma_all
    rz_1 = over_devices(kept * kept * a_all + alpha_0 * alpha_0 * g_all)
    beta = rz_1 / rz_0
    k = kept + beta
    curvature_1 = over_devices(
        k * k * c_all - alpha_0 * k * (f_all + g_all) + alpha_0 * alpha_0 * e_all
    )
    alpha_1 = rz_1 / curvature_1
    own_k = 1.0 - alpha_0 * view(packed, 5) + beta
    for i, row in enumerate((alpha_0 + alpha_1 * own_k, alpha_0 * alpha_1)):
        spread_row = jnp.where(lane == place, jnp.broadcast_to(row, (systems, lanes)), 0.0)
        coefs[i] = jnp.broadcast_to(
            jnp.sum(spread_row, axis=1, keepdims=True), (systems, lanes)
        )

    def close_send(offset, carry):
        send_to(offset).wait_send()
        return carry

    lax.fori_loop(1, group, close_send, 0)
    for dz, dy in DIRECTIONS:

        @pl.when(has(dz, dy))
        def _(dz=dz, dy=dy):
            label_copy(dz, dy).wait_send()
            halo_copy(dz, dy).wait_send()


def finish(
    r_ext, p_ext, q_ext, w_ext, y_own, coefs, solution_ref, residual_ref, out_s, out_r, out_sem
):
    systems, halves, depth, rows, lanes = y_own.shape
    own = slice(REACH, REACH + depth)
    copies = []
    for m in range(systems):
        main = coefs[0, m : m + 1, :][None]
        side = coefs[1, m : m + 1, :][None]
        for h in range(halves):
            cut = slice(h * lanes, (h + 1) * lanes)
            out_s[m, :, :, cut] = (
                main * p_ext[m, h, own, 0:rows, :] - side * w_ext[m, h, 1 : depth + 1, 0:rows, :]
            )
            out_r[m, :, :, cut] = (
                r_ext[h, own, 0:rows, :]
                - main * q_ext[m, h, 1 : depth + 1, 0:rows, :]
                + side * y_own[m, h]
            )
        for i, (source, target) in enumerate(((out_s, solution_ref), (out_r, residual_ref))):
            copies.append(pltpu.make_async_copy(source.at[m], target.at[m], out_sem.at[i, m]))
            copies[-1].start()
    for copy in copies:
        copy.wait()


def on_device(
    grid, right_side, labels, region_coeff, shift_index, shift_table, time_step, block_inverse
):
    depth, rows, nx = right_side.shape
    systems, lanes = block_inverse.shape[0], block_inverse.shape[1]
    halves = nx // lanes
    assert depth == EDGE and labels.shape[0] == 1
    group = grid[0] * grid[1]
    ring = rows + EDGE
    y_blocks = labels.shape[1]
    label_pad = -(-9 * y_blocks // 8) * 8
    f32 = jnp.float32
    vmem = pl.BlockSpec(memory_space=pltpu.VMEM)
    hbm = pl.BlockSpec(memory_space=pltpu.HBM)
    out = jax.ShapeDtypeStruct((systems,) + right_side.shape, f32)
    dma = pltpu.SemaphoreType.DMA
    tall, wide = depth + 2 * REACH, depth + 2
    fields = pl.pallas_call(
        functools.partial(kernel, grid),
        out_shape=tuple(
            jax.ShapeDtypeStruct(shape, f32)
            for shape in (
                (halves, tall, ring, lanes),
                (systems, halves, tall, ring, lanes),
                (systems, halves, wide, ring, lanes),
                (systems, halves, wide, ring, lanes),
                (systems, halves, depth, rows, lanes),
                (6, systems, lanes),
            )
        ),
        in_specs=[hbm] * 7,
        out_specs=(vmem,) * 6,
        scratch_shapes=[
            pltpu.VMEM(right_side.shape, f32),
            pltpu.VMEM(labels.shape, jnp.int32),
            pltpu.SMEM(region_coeff.shape, f32),
            pltpu.SMEM(shift_index.shape, jnp.int32),
            pltpu.SMEM(shift_table.shape, f32),
            pltpu.SMEM(time_step.shape, f32),
            pltpu.VMEM(block_inverse.shape, f32),
            pltpu.VMEM((systems, 2 * lanes, 2 * lanes), jnp.bfloat16),
            pltpu.VMEM((label_pad, nx), f32),
            pltpu.VMEM((label_pad, labels.shape[2]), f32),
            pltpu.VMEM((3, halves, ring, lanes), f32),
            pltpu.VMEM((5, halves, ring, lanes), f32),
            pltpu.VMEM((2, depth, REACH, nx), f32),
            pltpu.VMEM((2, REACH, rows, nx), f32),
            pltpu.VMEM((2, depth, REACH, nx), f32),
            pltpu.VMEM((2, 2, REACH, REACH, nx), f32),
            pltpu.VMEM((9,) + labels.shape, jnp.int32),
            pltpu.VMEM((1, lanes), f32),
            pltpu.VMEM((group, 1, lanes), f32),
            pltpu.VMEM((group, lanes), f32),
            dma((7,)),
            pltpu.SemaphoreType.REGULAR((max(1, max(grid) - 3),)),
            dma((9,)),
            dma((9,)),
            dma((9,)),
            dma((9,)),
            dma((group,)),
            dma((group,)),
        ],
        compiler_params=pltpu.CompilerParams(
            collective_id=0, has_side_effects=True, vmem_limit_bytes=32 * 1024 * 1024
        ),
    )(
        *(
            x if x is time_step else pltpu.with_memory_space_constraint(x, pltpu.HBM)
            for x in (
                right_side,
                labels,
                region_coeff,
                shift_index,
                shift_table,
                time_step,
                block_inverse,
            )
        )
    )
    return pl.pallas_call(
        finish,
        out_shape=(out, out),
        in_specs=[vmem] * 6,
        out_specs=(hbm, hbm),
        scratch_shapes=[pltpu.VMEM(out.shape, f32), pltpu.VMEM(out.shape, f32), dma((2, systems))],
        compiler_params=pltpu.CompilerParams(vmem_limit_bytes=32 * 1024 * 1024),
    )(*fields)


def solution(mesh):
    in_specs = (
        P(("sample", "gz"), "gy", None),
        P(("sample", "gz"), "gy", None),
        P("sample"),
        P("sample"),
        P(),
        P("sample"),
        P(),
    )
    out_specs = (P(None, ("sample", "gz"), "gy", None), P(None, ("sample", "gz"), "gy", None))
    grid = (mesh.shape["gz"], mesh.shape["gy"])
    return jax.shard_map(
        functools.partial(on_device, grid),
        mesh=mesh,
        in_specs=in_specs,
        out_specs=out_specs,
        check_vma=False,
    )
```

```python
import functools

import jax
import jax.numpy as jnp
from jax import lax
from jax.experimental import pallas as pl
from jax.experimental.pallas import tpu as pltpu
from jax.sharding import PartitionSpec as P

MESH = pl.DeviceIdType.MESH
EDGE = 8
REACH = 2
DIRECTIONS = [(dz, dy) for dz in (-1, 0, 1) for dy in (-1, 0, 1) if (dz, dy) != (0, 0)]


def slot(dz, dy):
    return (dz + 1) * 3 + dy + 1


def split(x):
    high = x.astype(jnp.bfloat16)
    low = (x - high.astype(jnp.float32)).astype(jnp.bfloat16)
    return high, low


def smooth_x(parts):
    width = parts[0].shape[1]
    lane = lax.broadcasted_iota(jnp.int32, parts[0].shape, 1)
    first, last = lane == 0, lane == width - 1
    rolled = [pltpu.roll(u, 1, 1) for u in parts]
    pairs = [
        u + jnp.where(first, rolled[i - 1] if i else 0.0, rolled[i]) for i, u in enumerate(parts)
    ]
    rolled = [pltpu.roll(h, width - 1, 1) for h in pairs]
    return [
        h + jnp.where(last, rolled[i + 1] if i + 1 < len(pairs) else parts[i], rolled[i])
        for i, h in enumerate(pairs)
    ]


def smooth_y(u):
    h = u + pltpu.roll(u, 1, 0)
    return h + pltpu.roll(h, u.shape[0] - 1, 0)


def smooth_xy(parts):
    return [smooth_y(u) for u in smooth_x(parts)]


def kernel(
    grid,
    right_hbm,
    labels_hbm,
    coeff_hbm,
    index_hbm,
    table_hbm,
    step_hbm,
    inverse_hbm,
    r_ext,
    p_ext,
    q_ext,
    w_ext,
    y_own,
    coefs,
    right_ref,
    labels_ref,
    coeff_ref,
    index_ref,
    table_ref,
    step_ref,
    inverse_ref,
    weights,
    c_rows,
    label_rows,
    c_planes,
    diag,
    y_send,
    z_recv,
    y_recv,
    corner_recv,
    label_recv,
    message,
    gathered,
    table,
    load_sem,
    near_sem,
    send_sem,
    recv_sem,
    label_send_sem,
    label_recv_sem,
    gather_send_sem,
    gather_recv_sem,
):
    n_gz, n_gy = grid
    group = n_gz * n_gy
    depth, rows, nx = right_ref.shape
    systems, lanes = inverse_ref.shape[0], inverse_ref.shape[1]
    halves = nx // lanes
    ring = r_ext.shape[2]
    y_blocks = labels_ref.shape[1]
    label_cols = labels_ref.shape[2]
    sample, gz, gy = lax.axis_index("sample"), lax.axis_index("gz"), lax.axis_index("gy")
    me = gz * n_gy + gy

    def has(dz, dy):
        z_ok = gz + dz >= 0 if dz < 0 else gz + dz < n_gz
        y_ok = gy + dy >= 0 if dy < 0 else gy + dy < n_gy
        return jnp.logical_and(z_ok, y_ok)

    def present(dz, dy):
        return jnp.where(has(dz, dy), 1.0, 0.0).astype(jnp.float32)

    def peer_of(offset):
        peer = lax.rem(me + offset, group)
        return peer, (sample, lax.div(peer, n_gy), lax.rem(peer, n_gy))

    loads = [
        pltpu.make_async_copy(source, target, load_sem.at[i])
        for i, (source, target) in enumerate(
            (
                (right_hbm, right_ref),
                (labels_hbm, labels_ref),
                (inverse_hbm, inverse_ref),
                (coeff_hbm, coeff_ref),
                (step_hbm, step_ref),
                (index_hbm, index_ref),
                (table_hbm, table_ref),
            )
        )
    ]
    for load in loads:
        load.start()

    z_recv[...] = jnp.zeros_like(z_recv)
    y_recv[...] = jnp.zeros_like(y_recv)
    corner_recv[...] = jnp.zeros_like(corner_recv)
    label_recv[...] = jnp.zeros_like(label_recv)

    barrier = pltpu.get_barrier_semaphore()

    def signal_near(semaphore):
        for dz, dy in DIRECTIONS:

            @pl.when(has(dz, dy))
            def _(dz=dz, dy=dy):
                pl.semaphore_signal(
                    semaphore,
                    inc=1,
                    device_id=(sample, gz + dz, gy + dy),
                    device_id_type=MESH,
                )

    z_near = 1 + (gz > 0).astype(jnp.int32) + (gz < n_gz - 1).astype(jnp.int32)
    y_near = 1 + (gy > 0).astype(jnp.int32) + (gy < n_gy - 1).astype(jnp.int32)
    near = z_near * y_near - 1

    signal_near(barrier)
    r_ext[...] = jnp.zeros_like(r_ext)
    loads[0].wait()
    loads[1].wait()
    y_send[0] = right_ref[:, 0:REACH, :]
    y_send[1] = right_ref[:, rows - REACH : rows, :]
    for h in range(halves):
        r_ext[h, REACH : REACH + depth, 0:rows, :] = right_ref[:, :, h * lanes : (h + 1) * lanes]

    pl.semaphore_wait(barrier, near)

    def halo_copy(dz, dy):
        device = (sample, gz + dz, gy + dy)
        z_from = depth - REACH if dz > 0 else 0
        if dy == 0:
            source = right_ref.at[pl.ds(z_from, REACH)]
            target = z_recv.at[0 if dz > 0 else 1]
        elif dz == 0:
            source = y_send.at[1 if dy > 0 else 0]
            target = y_recv.at[0 if dy > 0 else 1]
        else:
            source = y_send.at[1 if dy > 0 else 0, pl.ds(z_from, REACH)]
            target = corner_recv.at[0 if dz > 0 else 1, 0 if dy > 0 else 1]
        return pltpu.make_async_remote_copy(
            src_ref=source,
            dst_ref=target,
            send_sem=send_sem.at[slot(dz, dy)],
            recv_sem=recv_sem.at[slot(-dz, -dy)],
            device_id=device,
            device_id_type=MESH,
        )

    def label_copy(dz, dy):
        return pltpu.make_async_remote_copy(
            src_ref=labels_ref,
            dst_ref=label_recv.at[slot(-dz, -dy)],
            send_sem=label_send_sem.at[slot(dz, dy)],
            recv_sem=label_recv_sem.at[slot(-dz, -dy)],
            device_id=(sample, gz + dz, gy + dy),
            device_id_type=MESH,
        )

    for dz, dy in DIRECTIONS:

        @pl.when(has(dz, dy))
        def _(dz=dz, dy=dy):
            label_copy(dz, dy).start()
            halo_copy(dz, dy).start()

    for load in loads[2:]:
        load.wait()
    for m in range(systems):
        high, low = split(inverse_ref[m])
        weights[m, 0:lanes, 0:lanes] = high
        weights[m, lanes : 2 * lanes, 0:lanes] = high
        weights[m, 0:lanes, lanes : 2 * lanes] = low
        weights[m, lanes : 2 * lanes, lanes : 2 * lanes] = low

    def pieces(x):
        return jnp.concatenate(split(x.reshape(-1, lanes)), axis=1)

    def product(x, m):
        both = jnp.dot(x, weights[m], preferred_element_type=jnp.float32)
        return both[:, 0:lanes] + both[:, lanes : 2 * lanes]

    own_planes = slice(REACH, REACH + depth)
    own_pieces = pieces(r_ext[:, own_planes, 0:rows, :])
    for m in range(systems):
        p_ext[m, :, own_planes, 0:rows, :] = product(own_pieces, m).reshape(
            halves, depth, rows, lanes
        )

    for dz, dy in DIRECTIONS:

        @pl.when(has(dz, dy))
        def _(dz=dz, dy=dy):
            label_copy(-dz, -dy).wait_recv()
            halo_copy(-dz, -dy).wait_recv()

    rounds = max(n_gz, n_gy) - 3
    if rounds > 0:
        signal_near(near_sem.at[0])

    for h in range(halves):
        cut = slice(h * lanes, (h + 1) * lanes)
        for side in (0, 1):
            planes = slice(0, REACH) if side == 0 else slice(REACH + depth, 2 * REACH + depth)
            r_ext[h, planes, 0:rows, :] = z_recv[side, :, :, cut]
            r_ext[h, planes, rows : rows + REACH, :] = corner_recv[side, 1, :, :, cut]
            r_ext[h, planes, ring - REACH : ring, :] = corner_recv[side, 0, :, :, cut]
        own = slice(REACH, REACH + depth)
        r_ext[h, own, rows : rows + REACH, :] = y_recv[1, :, :, cut]
        r_ext[h, own, ring - REACH : ring, :] = y_recv[0, :, :, cut]

    label_rows[...] = jnp.zeros_like(label_rows)
    for s in range(9):
        near_labels = labels_ref[0] if s == slot(0, 0) else label_recv[s, 0]
        label_rows[s * y_blocks : (s + 1) * y_blocks, :] = near_labels.astype(jnp.float32)
    spread = jnp.where(
        lax.broadcasted_iota(jnp.int32, (label_cols, nx), 0)
        == lax.broadcasted_iota(jnp.int32, (label_cols, nx), 1) // EDGE,
        1.0,
        0.0,
    ).astype(jnp.bfloat16)
    wide = jnp.dot(
        label_rows[...].astype(jnp.bfloat16), spread, preferred_element_type=jnp.float32
    )
    cells = jnp.zeros_like(wide)
    scale = step_ref[0] * 0.125
    for region in range(coeff_ref.shape[0]):
        cells = jnp.where(wide == float(region), coeff_ref[region] * scale, cells)
    c_rows[...] = cells

    sub = lax.broadcasted_iota(jnp.int32, (EDGE, lanes), 0)
    for dz in (-1, 0, 1):
        for h in range(halves):
            cut = slice(h * lanes, (h + 1) * lanes)

            def row(dy, block):
                at = slot(dz, dy) * y_blocks + block
                value = c_rows[at : at + 1, cut]
                if (dz, dy) != (0, 0):
                    value = value * present(dz, dy)
                return jnp.broadcast_to(value, (EDGE, lanes))

            for block in range(y_blocks):
                c_planes[dz + 1, h, block * EDGE : (block + 1) * EDGE, :] = row(0, block)
            c_planes[dz + 1, h, rows:ring, :] = jnp.where(
                sub < EDGE // 2, row(1, 0), row(-1, y_blocks - 1)
            )

    for h in range(halves):
        c_planes[3, h] = pltpu.roll(c_planes[1, h], 1, 0)
        c_planes[4, h] = pltpu.roll(c_planes[1, h], ring - 1, 0)

    smooth = [smooth_xy([c_planes[d, h] for h in range(halves)]) for d in range(3)]
    for h in range(halves):
        low, own, high = (smooth[d][h] for d in range(3))
        diag[0, h] = 3.0 * low + own + 64.0 * c_planes[0, h]
        diag[1, h] = low + 3.0 * own + 64.0 * c_planes[1, h]
        diag[2, h] = 4.0 * own + 64.0 * c_planes[1, h]
        diag[3, h] = high + 3.0 * own + 64.0 * c_planes[1, h]
        diag[4, h] = 3.0 * high + own + 64.0 * c_planes[2, h]

    ring_row = lax.broadcasted_iota(jnp.int32, (ring, lanes), 0)
    row_mask = jnp.where(
        ring_row < rows,
        1.0,
        jnp.where(ring_row < rows + EDGE // 2, present(0, 1), present(0, -1)),
    )

    def apply(field, z, shift):
        def c_of(plane):
            return 0 if plane < 0 else 2 if plane >= depth else 1

        below, here, above = field(z - 1), field(z), field(z + 1)
        kind = 0 if z < 0 else 4 if z >= depth else 1 if z == 0 else 3 if z == depth - 1 else 2
        ku, kcu = [], []
        for h in range(halves):
            u = (below[h] + here[h]) + (here[h] + above[h])
            if kind == 2:
                twice = u + u
                before, after = pltpu.roll(u, 1, 0), pltpu.roll(u, ring - 1, 0)
                u = twice + before + after
                cu = (
                    c_planes[1, h] * twice
                    + c_planes[3, h] * before
                    + c_planes[4, h] * after
                )
            else:
                cu = (
                    c_planes[c_of(z - 1), h] * below[h]
                    + 2.0 * (c_planes[c_of(z), h] * here[h])
                    + c_planes[c_of(z + 1), h] * above[h]
                )
            ku.append(u)
            kcu.append(cu)
        along = smooth_x if kind == 2 else smooth_xy
        ku, kcu = along(ku), along(kcu)
        return [
            (diag[kind, h] + shift) * here[h] - c_planes[c_of(z), h] * ku[h] - kcu[h]
            for h in range(halves)
        ]

    def fold(total, term):
        term = term.reshape(-1, 8, lanes)
        for i in range(term.shape[0]):
            total = total + term[i]
        return total

    def put(quantity, m, total):
        value = jnp.sum(jnp.sum(total, axis=0, keepdims=True), axis=1, keepdims=True)
        coefs[quantity, pl.ds(m, 1), :] = jnp.broadcast_to(value, (1, lanes))

    zero = jnp.zeros((8, lanes), jnp.float32)

    z_pieces = [
        pieces(r_ext[:, planes])
        for planes in (slice(0, REACH), slice(REACH + depth, 2 * REACH + depth))
    ]
    y_pieces = pieces(r_ext[:, own_planes, rows:ring, :])
    for m in range(systems):
        for planes, x in zip(
            (slice(0, REACH), slice(REACH + depth, 2 * REACH + depth)), z_pieces
        ):
            p_ext[m, :, planes] = product(x, m).reshape(halves, REACH, ring, lanes)
        p_ext[m, :, own_planes, rows:ring, :] = product(y_pieces, m).reshape(
            halves, depth, ring - rows, lanes
        )

    def first(m, carry):
        shift = table_ref[index_ref[m]]
        a, c = zero, zero
        for z in range(-1, depth + 1):
            image = apply(
                lambda k: [p_ext[m, h, k + REACH] for h in range(halves)], z, shift
            )
            for h in range(halves):
                value = image[h] * row_mask
                if z < 0:
                    value = value * present(-1, 0)
                elif z >= depth:
                    value = value * present(1, 0)
                else:
                    p = p_ext[m, h, z + REACH, 0:rows, :]
                    a = fold(a, p * r_ext[h, z + REACH, 0:rows, :])
                    c = fold(c, p * value[0:rows])
                q_ext[m, h, z + 1] = value
        put(0, m, a)
        put(1, m, c)
        return carry

    lax.fori_loop(0, systems, first, 0)

    a_own, c_own = coefs[0], coefs[1]
    sigma = jnp.where(a_own > 0.0, c_own / jnp.where(a_own > 0.0, a_own, 1.0), 0.0)
    coefs[5] = sigma

    def second(m, carry):
        shift = table_ref[index_ref[m]]
        s_row = coefs[5, pl.ds(m, 1), :]
        q_shifted = q_ext[m] - s_row[None, None] * r_ext[:, 1 : REACH + depth + 1]
        w_ext[m] = product(pieces(q_shifted), m).reshape(q_shifted.shape)
        g, f, e = zero, zero, zero
        for z in range(depth):
            image = apply(lambda k: [w_ext[m, h, k + 1] for h in range(halves)], z, shift)
            for h in range(halves):
                y = image[h][0:rows]
                w = w_ext[m, h, z + 1, 0:rows, :]
                q = q_ext[m, h, z + 1, 0:rows, :] - s_row * r_ext[h, z + REACH, 0:rows, :]
                g = fold(g, w * q)
                f = fold(f, p_ext[m, h, z + REACH, 0:rows, :] * y)
                e = fold(e, w * y)
                y_own[m, h, z] = y
        put(2, m, g)
        put(3, m, f)
        put(4, m, e)
        return carry

    lax.fori_loop(0, systems, second, 0)

    for r in range(rounds):
        pl.semaphore_wait(near_sem.at[r], near)
        if r + 1 < rounds:
            signal_near(near_sem.at[r + 1])

    lane = lax.broadcasted_iota(jnp.int32, (systems, lanes), 1)
    place = lax.broadcasted_iota(jnp.int32, (systems, lanes), 0)
    packed = jnp.zeros((systems, lanes), jnp.float32)
    for quantity in range(6):
        packed = jnp.where(lane == place + quantity * systems, coefs[quantity], packed)
    packed = jnp.sum(packed, axis=0, keepdims=True)
    message[...] = packed

    def gather_copy(device, source):
        return pltpu.make_async_remote_copy(
            src_ref=message,
            dst_ref=gathered.at[source],
            send_sem=gather_send_sem.at[source],
            recv_sem=gather_recv_sem.at[source],
            device_id=device,
            device_id_type=MESH,
        )

    def send_to(offset):
        peer, device = peer_of(offset)
        return pltpu.make_async_remote_copy(
            src_ref=message,
            dst_ref=gathered.at[me],
            send_sem=gather_send_sem.at[peer],
            recv_sem=gather_recv_sem.at[me],
            device_id=device,
            device_id_type=MESH,
        )

    def send_step(offset, carry):
        send_to(offset).start()
        return carry

    lax.fori_loop(1, group, send_step, 0)

    def receive_step(offset, carry):
        peer, device = peer_of(offset)
        gather_copy(device, peer).wait_recv()
        return carry

    lax.fori_loop(1, group, receive_step, 0)

    gathered[me] = packed
    for source in range(group):
        table[source : source + 1, :] = gathered[source]

    def view(rows_of, quantity):
        return pltpu.roll(rows_of, lanes - quantity * systems, 1) if quantity else rows_of

    def over_devices(x):
        return jnp.sum(x, axis=0, keepdims=True)

    everyone = table[...]
    a_all, c_all, g_all, f_all, e_all, sigma_all = (view(everyone, i) for i in range(6))
    rz_0 = over_devices(a_all)
    alpha_0 = rz_0 / over_devices(c_all)
    kept = 1.0 - alpha_0 * sigma_all
    rz_1 = over_devices(kept * kept * a_all + alpha_0 * alpha_0 * g_all)
    beta = rz_1 / rz_0
    k = kept + beta
    curvature_1 = over_devices(
        k * k * c_all - alpha_0 * k * (f_all + g_all) + alpha_0 * alpha_0 * e_all
    )
    alpha_1 = rz_1 / curvature_1
    own_k = 1.0 - alpha_0 * view(packed, 5) + beta
    for i, row in enumerate((alpha_0 + alpha_1 * own_k, alpha_0 * alpha_1)):
        spread_row = jnp.where(lane == place, jnp.broadcast_to(row, (systems, lanes)), 0.0)
        coefs[i] = jnp.broadcast_to(
            jnp.sum(spread_row, axis=1, keepdims=True), (systems, lanes)
        )

    def close_send(offset, carry):
        send_to(offset).wait_send()
        return carry

    lax.fori_loop(1, group, close_send, 0)
    for dz, dy in DIRECTIONS:

        @pl.when(has(dz, dy))
        def _(dz=dz, dy=dy):
            label_copy(dz, dy).wait_send()
            halo_copy(dz, dy).wait_send()


def finish(
    r_ext, p_ext, q_ext, w_ext, y_own, coefs, solution_ref, residual_ref, out_s, out_r, out_sem
):
    systems, halves, depth, rows, lanes = y_own.shape
    own = slice(REACH, REACH + depth)
    copies = []
    for m in range(systems):
        main = coefs[0, m : m + 1, :][None]
        side = coefs[1, m : m + 1, :][None]
        for h in range(halves):
            cut = slice(h * lanes, (h + 1) * lanes)
            out_s[m, :, :, cut] = (
                main * p_ext[m, h, own, 0:rows, :] - side * w_ext[m, h, 1 : depth + 1, 0:rows, :]
            )
            out_r[m, :, :, cut] = (
                r_ext[h, own, 0:rows, :]
                - main * q_ext[m, h, 1 : depth + 1, 0:rows, :]
                + side * y_own[m, h]
            )
        for i, (source, target) in enumerate(((out_s, solution_ref), (out_r, residual_ref))):
            copies.append(pltpu.make_async_copy(source.at[m], target.at[m], out_sem.at[i, m]))
            copies[-1].start()
    for copy in copies:
        copy.wait()


def on_device(
    grid, right_side, labels, region_coeff, shift_index, shift_table, time_step, block_inverse
):
    depth, rows, nx = right_side.shape
    systems, lanes = block_inverse.shape[0], block_inverse.shape[1]
    halves = nx // lanes
    assert depth == EDGE and labels.shape[0] == 1
    group = grid[0] * grid[1]
    ring = rows + EDGE
    y_blocks = labels.shape[1]
    label_pad = -(-9 * y_blocks // 8) * 8
    f32 = jnp.float32
    vmem = pl.BlockSpec(memory_space=pltpu.VMEM)
    hbm = pl.BlockSpec(memory_space=pltpu.HBM)
    out = jax.ShapeDtypeStruct((systems,) + right_side.shape, f32)
    dma = pltpu.SemaphoreType.DMA
    tall, wide = depth + 2 * REACH, depth + 2
    fields = pl.pallas_call(
        functools.partial(kernel, grid),
        out_shape=tuple(
            jax.ShapeDtypeStruct(shape, f32)
            for shape in (
                (halves, tall, ring, lanes),
                (systems, halves, tall, ring, lanes),
                (systems, halves, wide, ring, lanes),
                (systems, halves, wide, ring, lanes),
                (systems, halves, depth, rows, lanes),
                (6, systems, lanes),
            )
        ),
        in_specs=[hbm] * 7,
        out_specs=(vmem,) * 6,
        scratch_shapes=[
            pltpu.VMEM(right_side.shape, f32),
            pltpu.VMEM(labels.shape, jnp.int32),
            pltpu.SMEM(region_coeff.shape, f32),
            pltpu.SMEM(shift_index.shape, jnp.int32),
            pltpu.SMEM(shift_table.shape, f32),
            pltpu.SMEM(time_step.shape, f32),
            pltpu.VMEM(block_inverse.shape, f32),
            pltpu.VMEM((systems, 2 * lanes, 2 * lanes), jnp.bfloat16),
            pltpu.VMEM((label_pad, nx), f32),
            pltpu.VMEM((label_pad, labels.shape[2]), f32),
            pltpu.VMEM((5, halves, ring, lanes), f32),
            pltpu.VMEM((5, halves, ring, lanes), f32),
            pltpu.VMEM((2, depth, REACH, nx), f32),
            pltpu.VMEM((2, REACH, rows, nx), f32),
            pltpu.VMEM((2, depth, REACH, nx), f32),
            pltpu.VMEM((2, 2, REACH, REACH, nx), f32),
            pltpu.VMEM((9,) + labels.shape, jnp.int32),
            pltpu.VMEM((1, lanes), f32),
            pltpu.VMEM((group, 1, lanes), f32),
            pltpu.VMEM((group, lanes), f32),
            dma((7,)),
            pltpu.SemaphoreType.REGULAR((max(1, max(grid) - 3),)),
            dma((9,)),
            dma((9,)),
            dma((9,)),
            dma((9,)),
            dma((group,)),
            dma((group,)),
        ],
        compiler_params=pltpu.CompilerParams(
            collective_id=0, has_side_effects=True, vmem_limit_bytes=32 * 1024 * 1024
        ),
    )(
        *(
            x if x is time_step else pltpu.with_memory_space_constraint(x, pltpu.HBM)
            for x in (
                right_side,
                labels,
                region_coeff,
                shift_index,
                shift_table,
                time_step,
                block_inverse,
            )
        )
    )
    return pl.pallas_call(
        finish,
        out_shape=(out, out),
        in_specs=[vmem] * 6,
        out_specs=(hbm, hbm),
        scratch_shapes=[pltpu.VMEM(out.shape, f32), pltpu.VMEM(out.shape, f32), dma((2, systems))],
        compiler_params=pltpu.CompilerParams(vmem_limit_bytes=32 * 1024 * 1024),
    )(*fields)


def solution(mesh):
    in_specs = (
        P(("sample", "gz"), "gy", None),
        P(("sample", "gz"), "gy", None),
        P("sample"),
        P("sample"),
        P(),
        P("sample"),
        P(),
    )
    out_specs = (P(None, ("sample", "gz"), "gy", None), P(None, ("sample", "gz"), "gy", None))
    grid = (mesh.shape["gz"], mesh.shape["gy"])
    return jax.shard_map(
        functools.partial(on_device, grid),
        mesh=mesh,
        in_specs=in_specs,
        out_specs=out_specs,
        check_vma=False,
    )
```
